32 devices in a mesh: tp: 4 (over y, x), dp: 8 (over z, core).
Axes of the slice: x: 2, y: 2, z: 4, core: 2. Of those that a mesh axis runs over, the one named last changes fastest.
Arguments:
- activations: bfloat16 [2, 8192, 8192], P(None, 'dp', 'tp'), may hold values from -72 to 72
- out_grads: bfloat16 [2, 8192, 2048], P(None, 'dp'), may hold values from -2 to 2
- master: float32 [8192, 2, 2048], P(('tp', 'dp')), may hold values from -1.2 to 1.2
- first_moment: float32 [8192, 2, 2048], P(('tp', 'dp')), may hold values from -1.8 to 1.8
- second_moment: float32 [8192, 2, 2048], P(('tp', 'dp')), may hold values from 0.01 to 1
Outputs:
- new_master: float32 [8192, 2, 2048], P(('tp', 'dp'))
- new_first: float32 [8192, 2, 2048], P(('tp', 'dp'))
- new_second: float32 [8192, 2, 2048], P(('tp', 'dp'))
- weights: bfloat16 [8192, 2, 2048], P('tp')
The draws below stay inside these ranges and needn't reach their ends.
All inputs are finite; a program needn't handle non-finite values.
Results may differ from the reference program's by a relative error of at most 0.0004.
Values may be sent and summed in bfloat16 or wider, within the bound.
A program may use at most 192 MiB of HBM per device.

```python
import math
import jax
import jax.numpy as jnp

D = 8192
KVW = 2048
LAYERS = 2
TOKENS = 8192


def shared_signs(key):
    sign_bits = jax.random.randint(jax.random.fold_in(key, 101), (LAYERS, TOKENS), 0, 2)
    return (2 * sign_bits - 1).astype(jnp.float32)


def draw_activations(key, part):
    token_signs = shared_signs(key)
    noise_key = jax.random.fold_in(key, 202)
    along_key = jax.random.fold_in(key, 203)
    noise = jnp.clip(jax.random.normal(noise_key, (LAYERS, TOKENS, D), jnp.float32), -6.0, 6.0)
    direction = jnp.clip(jax.random.normal(along_key, (LAYERS, D), jnp.float32), -3.0, 3.0)
    strength = 8.0
    values = 8.0 * noise + strength * token_signs[:, :, None] * direction[:, None, :]
    return values.astype(jnp.bfloat16)


def draw_out_grads(key, part):
    token_signs = shared_signs(key)
    noise_key = jax.random.fold_in(key, 302)
    along_key = jax.random.fold_in(key, 303)
    noise = jnp.clip(jax.random.normal(noise_key, (LAYERS, TOKENS, KVW), jnp.float32), -6.0, 6.0)
    direction = jnp.clip(jax.random.normal(along_key, (LAYERS, KVW), jnp.float32), -3.0, 3.0)
    values = noise * TOKENS ** (-0.5) + token_signs[:, :, None] * direction[:, None, :] * (1.0 / TOKENS)
    return values.astype(jnp.bfloat16)


def block_scale(own_key, shape, split, smallest, high):
    factor_of = 1.0
    for dim, blocks in split:
        steps = jax.random.uniform(jax.random.fold_in(jax.random.fold_in(own_key, 6), dim), (blocks,), jnp.float32, smallest / len(split), high / len(split))
        factor_of = factor_of * jnp.repeat(jnp.exp(steps), shape[dim] // blocks).reshape((-1,) + (1,) * (len(shape) - 1 - dim))
    return factor_of


def centred(key, dims, width, reach, pieces=(), dtype=jnp.bfloat16):
    values = width * jax.random.normal(key, dims, jnp.float32)
    if pieces:
        values = values * block_scale(key, dims, pieces, -0.22, 0.18)
    return jnp.clip(values, -reach, reach).astype(dtype)


def setup_inputs(seed: int = 0) -> dict:
    keys = jax.random.split(jax.random.key(seed), 6)
    return {
        "activations": draw_activations(jax.random.fold_in(keys[5], 71), 0),
        "out_grads": draw_out_grads(jax.random.fold_in(keys[5], 71), 0),
        "master": centred(keys[2], (D, LAYERS, KVW), 0.2, 1.2, ((0, 32),), jnp.float32),
        "first_moment": centred(keys[3], (D, LAYERS, KVW), 0.3, 1.8, ((0, 32),), jnp.float32),
        "second_moment": jnp.clip(jnp.exp(math.log(1.0) - 4.6051702 * jax.random.uniform(keys[4], (D, LAYERS, KVW), jnp.float32) ** block_scale(keys[4], (D, LAYERS, KVW), ((0, 32),), -0.2, 0.2)), 0.01, 1.0),
    }


beta_first = 0.9
beta_second = 0.95
first_fix = 1.0 - 0.9 ** 10
second_fix = 1.0 - 0.95 ** 10
learn_rate = 0.01
decay_rate = 0.1
epsilon = 1e-08
limit_scale = 2.0

def reference(activations, out_grads, master, first_moment, second_moment):
    grad = jnp.einsum('ltd,ltc->dlc', activations.astype(jnp.float32), out_grads.astype(jnp.float32))
    squares = jnp.sum(grad * grad)
    limit = limit_scale * math.sqrt(D * LAYERS * KVW)
    clip_factor = limit / jnp.maximum(jnp.sqrt(squares), limit)
    clipped = clip_factor * grad
    new_first = beta_first * first_moment + (1.0 - beta_first) * clipped
    new_second = beta_second * second_moment + (1.0 - beta_second) * clipped * clipped
    step_dir = new_first / first_fix / (jnp.sqrt(new_second / second_fix) + epsilon)
    new_master = master - learn_rate * (step_dir + decay_rate * master)
    return (new_master, new_first, new_second, new_master.astype(jnp.bfloat16))
```

```python
import functools
import math

import jax
import jax.numpy as jnp
from jax import lax
from jax.experimental import pallas as pl
from jax.experimental.pallas import tpu as pltpu
from jax.sharding import PartitionSpec as P

beta_first = 0.9
beta_second = 0.95
first_fix = 1.0 - 0.9**10
second_fix = 1.0 - 0.95**10
learn_rate = 0.01
decay_rate = 0.1
epsilon = 1e-08
limit_scale = 2.0
MESH = pl.DeviceIdType.MESH
CORES = 2
LANES = 128
TILE = 16
TOP = 224.0
STATE_SLOTS = 4


def decode(code, scale):
    code = code.astype(jnp.float32)
    size = jnp.abs(code)
    root = jnp.exp(jnp.log(jnp.maximum(size, 1e-37)) * (1.0 / 16.0))
    root = jnp.where(size > 0.0, root, 0.0)
    return jnp.where(code < 0.0, -root, root) * scale


def encode(value, shrink):
    x = value * shrink
    power = x * x
    power = power * power
    power = power * power
    power = power * power
    return jnp.where(x < 0.0, -power, power).astype(jnp.bfloat16)


def step_kernel(
    d,
    acts, grads, master, first, second,
    new_master, new_first, new_second, weights,
    a_buf, b_buf, part, rx, grad, wide, state, norm,
    a_own, a_send, a_recv, b_own, b_send, b_recv,
    rs_send, rs_recv, norm_send, norm_recv, state_in, state_out,
    ag_send, ag_recv, out_local, out_send, out_recv,
):
    L, T, R, N, C, AW, WC, NB = d.L, d.T, d.R, d.N, d.C, d.AW, d.WC, d.NB
    n_tp, n_dp = d.n_tp, d.n_dp
    pieces, tiles_across, lane_tiles = L * NB, WC // LANES, N // LANES
    tiles = R // TILE * tiles_across
    stride = lane_tiles * L
    index = lax.axis_index("dp")
    chip, core = index // CORES, lax.rem(index, CORES)
    partner = {"dp": chip * CORES + 1 - core}
    me = lax.axis_index("tp") * n_dp + index
    count = n_tp * n_dp

    def column(c, k):
        start = c * CORES * R + (k * R if AW == R else 0)
        return pl.ds(pl.multiple_of(start, LANES), AW)

    def a_local(l, c):
        return pltpu.make_async_copy(
            acts.at[l, :, column(c, core)], a_buf.at[0, l, c], a_own.at[l, c]
        )

    def a_remote(l, c):
        return pltpu.make_async_remote_copy(
            acts.at[l, :, column(c, 1 - core)], a_buf.at[1, l, c],
            a_send.at[l, c], a_recv.at[l, c],
            device_id=partner, device_id_type=MESH,
        )

    def b_columns(j):
        return pl.ds(pl.multiple_of(j * WC, LANES), WC)

    def b_local(l, j):
        return pltpu.make_async_copy(
            grads.at[l, :, b_columns(j)], b_buf.at[0, l, j], b_own.at[l, j]
        )

    def b_remote(l, j):
        return pltpu.make_async_remote_copy(
            grads.at[l, :, b_columns(j)], b_buf.at[1, l, j],
            b_send.at[l, j], b_recv.at[l, j],
            device_id=partner, device_id_type=MESH,
        )

    def in_order(a_copy, b_copy):
        for l in range(L):
            a_copy(l, C - 1).start()
            a_copy(l, 0).start()
            for j in range(NB):
                b_copy(l, j).start()
            for c in range(1, C - 1):
                a_copy(l, c).start()

    in_order(a_local, b_local)

    rows_q = d.rows_q
    sources = (master, first, second)
    targets = (new_master, new_first, new_second)

    def state_load(i, q):
        slot = lax.rem(q, STATE_SLOTS)
        return pltpu.make_async_copy(
            sources[i].at[pl.ds(q * rows_q, rows_q)], state.at[i, slot], state_in.at[i, slot]
        )

    def state_store(i, q):
        slot = lax.rem(q, STATE_SLOTS)
        return pltpu.make_async_copy(
            state.at[i, slot], targets[i].at[pl.ds(q * rows_q, rows_q)], state_out.at[i, slot]
        )

    barrier = pltpu.get_barrier_semaphore()

    def device(k):
        other = lax.rem(me + k, count)
        return {"tp": other // n_dp, "dp": lax.rem(other, n_dp)}

    @pl.loop(1, count)
    def _(k):
        pl.semaphore_signal(barrier, inc=1, device_id=device(k), device_id_type=MESH)

    pl.semaphore_wait(barrier, count - 1)

    in_order(a_remote, b_remote)

    for q in range(min(STATE_SLOTS, d.PQ)):
        for i in range(3):
            state_load(i, jnp.int32(q)).start()

    def product(c, l, j):
        total = None
        for w in range(CORES):
            lhs = a_buf[w, l, c]
            if AW != R:
                lhs = jnp.where(core == 0, lhs[:, :R], lhs[:, R:])
            term = lax.dot_general(
                lhs, b_buf[w, l, j], (((0,), (0,)), ((), ())),
                preferred_element_type=jnp.float32,
            )
            total = term if total is None else total + term
        part[...] = total

    def rs_copy(way, s, p):
        to = chip + 1 if way == 0 else chip - 1
        return pltpu.make_async_remote_copy(
            rx.at[way, s, p], rx.at[way, s, p],
            rs_send.at[way, s, p], rs_recv.at[way, s, p],
            device_id={"dp": to * CORES + core}, device_id_type=MESH,
        )

    def add_received(way, s, p):
        rs_copy(way, s, p).wait_recv()
        scale = rx[way, s, p, tiles].astype(jnp.float32) * (1.0 / TOP)

        @pl.loop(0, R // TILE)
        def _(r):
            rows = pl.ds(pl.multiple_of(r * TILE, TILE), TILE)
            for t in range(tiles_across):
                lanes = pl.ds(t * LANES, LANES)
                code = rx[way, s, p, r * tiles_across + t]
                part[rows, lanes] += decode(code, scale)

    def send_on(way, s, p):
        def widest(r, top):
            rows = pl.ds(pl.multiple_of(r * TILE, TILE), TILE)
            for t in range(tiles_across):
                top = jnp.maximum(top, jnp.abs(part[rows, pl.ds(t * LANES, LANES)]))
            return top

        top = lax.fori_loop(0, R // TILE, widest, jnp.zeros((TILE, LANES), jnp.float32))
        top = jnp.maximum(top, 1e-25).astype(jnp.bfloat16)
        rx[way, s, p, tiles] = top
        shrink = TOP / top.astype(jnp.float32)

        @pl.loop(0, R // TILE)
        def _(r):
            rows = pl.ds(pl.multiple_of(r * TILE, TILE), TILE)
            for t in range(tiles_across):
                value = part[rows, pl.ds(t * LANES, LANES)]
                rx[way, s, p, r * tiles_across + t] = encode(value, shrink)

        rs_copy(way, s, p).start()

    def own_rows(r, l, j, t, half):
        start = ((r * TILE + half * 8) * lane_tiles + j * tiles_across + t) * L + l
        return pl.ds(start, 8, stride=stride)

    def keep_own(l, j):
        @pl.loop(0, R // TILE)
        def _(r):
            rows = pl.ds(pl.multiple_of(r * TILE, TILE), TILE)
            for t in range(tiles_across):
                value = part[rows, pl.ds(t * LANES, LANES)]
                for half in range(2):
                    grad[own_rows(r, l, j, t, half), :] = value[half * 8 : half * 8 + 8]

    def add_own(way, s, p, l, j):
        rs_copy(way, s, p).wait_recv()
        scale = rx[way, s, p, tiles].astype(jnp.float32) * (1.0 / TOP)

        @pl.loop(0, R // TILE)
        def _(r):
            for t in range(tiles_across):
                value = decode(rx[way, s, p, r * tiles_across + t], scale)
                for half in range(2):
                    where = own_rows(r, l, j, t, half)
                    grad[where, :] = grad[where, :] + value[half * 8 : half * 8 + 8]

    @pl.loop(0, C)
    def _(s):
        high, low = C - 1 - s, s

        @pl.loop(0, pieces)
        def _(p):
            l, j = p // NB, lax.rem(p, NB)

            @pl.when(s == 0)
            def _():
                @pl.when(j == 0)
                def _():
                    for c in sorted({0, C - 1}):
                        a_local(l, c).wait()
                        a_remote(l, c).wait_recv()

                b_local(l, j).wait()
                b_remote(l, j).wait_recv()

            @pl.when((s < C - 1) & (chip < high))
            def _():
                product(high, l, j)

                @pl.when(chip > 0)
                def _():
                    add_received(0, s, p)

                send_on(0, s, p)

            @pl.when((s < C - 1) & (chip > low))
            def _():
                product(low, l, j)

                @pl.when(chip < C - 1)
                def _():
                    add_received(1, s, p)

                send_on(1, s, p)

            @pl.when(s == 0)
            def _():
                @pl.when(j == 0)
                def _():
                    for c in range(1, C - 1):
                        a_local(l, c).wait()
                        a_remote(l, c).wait_recv()

                product(chip, l, j)
                keep_own(l, j)

            @pl.when((s > 0) & (chip == C - s) & (chip > 0))
            def _():
                add_own(0, s - 1, p, l, j)

            @pl.when((s > 0) & (chip == s - 1) & (chip < C - 1))
            def _():
                add_own(1, s - 1, p, l, j)

    own_total = R * stride
    block = 64

    def square(b, sums):
        x = grad[pl.ds(pl.multiple_of(b * block, block), block), :]
        x = x * x
        for i in range(block // 8):
            sums = sums + x[i * 8 : i * 8 + 8]
        return sums

    sums = lax.fori_loop(0, own_total // block, square, jnp.zeros((8, LANES), jnp.float32))
    norm[me] = jnp.sum(sums, axis=0, keepdims=True)

    def norm_copy(k, slot):
        return pltpu.make_async_remote_copy(
            norm.at[slot], norm.at[slot], norm_send.at[k], norm_recv.at[k],
            device_id=device(k), device_id_type=MESH,
        )

    @pl.loop(1, count)
    def _(k):
        norm_copy(k, me).start()

    @pl.loop(1, count)
    def _(k):
        norm_copy(k, lax.rem(me - k + count, count)).wait_recv()

    total = jnp.sum(jnp.sum(norm[...], axis=0), axis=1, keepdims=True)
    limit = limit_scale * math.sqrt(own_total * LANES * count)
    clip = limit / jnp.maximum(jnp.sqrt(total), limit)
    clip = jnp.broadcast_to(clip, (block, LANES))

    def place(c, q):
        start = (c * CORES + core) * own_total + q * rows_q
        return pl.ds(pl.multiple_of(start, TILE), rows_q)

    def ag_copy(way, c, q):
        to = chip + 1 if way == 0 else chip - 1
        return pltpu.make_async_remote_copy(
            wide.at[c, q], wide.at[c, q], ag_send.at[way, c, q], ag_recv.at[c, q],
            device_id={"dp": to * CORES + core}, device_id_type=MESH,
        )

    def local_copy(c, q):
        return pltpu.make_async_copy(wide.at[c, q], weights.at[place(c, q)], out_local.at[c, q])

    def partner_copy(c, q):
        return pltpu.make_async_remote_copy(
            wide.at[c, q], weights.at[place(c, q)], out_send.at[c, q], out_recv.at[c, q],
            device_id=partner, device_id_type=MESH,
        )

    def partner_place(c, q):
        start = (c * CORES + 1 - core) * own_total + q * rows_q
        return pl.ds(pl.multiple_of(start, TILE), rows_q)

    def partner_arrival(c, q):
        return pltpu.make_async_remote_copy(
            wide.at[c, q], weights.at[partner_place(c, q)], out_send.at[c, q], out_recv.at[c, q],
            device_id=partner, device_id_type=MESH,
        )

    @pl.loop(0, d.PQ)
    def _(q):
        slot = lax.rem(q, STATE_SLOTS)
        for i in range(3):
            state_load(i, q).wait()

        @pl.loop(0, rows_q // block)
        def _(b):
            here = pl.ds(pl.multiple_of(b * block, block), block)
            there = pl.ds(pl.multiple_of(q * rows_q + b * block, block), block)
            clipped = clip * grad[there, :]
            moment = beta_first * state[1, slot, here, :] + (1.0 - beta_first) * clipped
            spread = beta_second * state[2, slot, here, :]
            spread = spread + (1.0 - beta_second) * clipped * clipped
            old = state[0, slot, here, :]
            direction = moment / first_fix / (jnp.sqrt(spread / second_fix) + epsilon)
            new = old - learn_rate * (direction + decay_rate * old)
            state[0, slot, here, :] = new
            state[1, slot, here, :] = moment
            state[2, slot, here, :] = spread
            wide[chip, q, here, :] = new.astype(jnp.bfloat16)

        @pl.when(chip > 0)
        def _():
            ag_copy(1, chip, q).start()

        @pl.when(chip < C - 1)
        def _():
            ag_copy(0, chip, q).start()

        for i in range(3):
            state_store(i, q).start()
        local_copy(chip, q).start()
        partner_copy(chip, q).start()

        @pl.when((q > 0) & (q - 1 + STATE_SLOTS < d.PQ))
        def _():
            for i in range(3):
                state_store(i, q - 1).wait()
                state_load(i, q - 1 + STATE_SLOTS).start()

    @pl.loop(1, C)
    def _(far):
        @pl.loop(0, d.PQ)
        def _(q):
            @pl.when(chip - far >= 0)
            def _():
                ag_copy(0, chip - far, q).wait_recv()

                @pl.when(chip < C - 1)
                def _():
                    ag_copy(0, chip - far, q).start()

                local_copy(chip - far, q).start()
                partner_copy(chip - far, q).start()

            @pl.when(chip + far < C)
            def _():
                ag_copy(1, chip + far, q).wait_recv()

                @pl.when(chip > 0)
                def _():
                    ag_copy(1, chip + far, q).start()

                local_copy(chip + far, q).start()
                partner_copy(chip + far, q).start()

    for q in range(max(0, d.PQ - STATE_SLOTS), d.PQ):
        for i in range(3):
            state_store(i, jnp.int32(q)).wait()

    for l in range(L):
        for c in range(C):
            a_remote(l, c).wait_send()
        for j in range(NB):
            b_remote(l, j).wait_send()

    @pl.loop(1, count)
    def _(k):
        norm_copy(k, me).wait_send()

    @pl.loop(0, C - 1)
    def _(s):
        @pl.loop(0, pieces)
        def _(p):
            @pl.when(chip < C - 1 - s)
            def _():
                rs_copy(0, s, p).wait_send()

            @pl.when(chip > s)
            def _():
                rs_copy(1, s, p).wait_send()

    @pl.loop(0, C)
    def _(c):
        @pl.loop(0, d.PQ)
        def _(q):
            @pl.when((c <= chip) & (chip < C - 1))
            def _():
                ag_copy(0, c, q).wait_send()

            @pl.when((c >= chip) & (chip > 0))
            def _():
                ag_copy(1, c, q).wait_send()

            local_copy(c, q).wait()
            partner_copy(c, q).wait_send()
            partner_arrival(c, q).wait_recv()


class Sizes:
    pass


def whole_step(acts, grads, master, first, second):
    d = Sizes()
    d.L, d.T, width = acts.shape
    d.N = grads.shape[2]
    d.n_tp, d.n_dp = lax.axis_size("tp"), lax.axis_size("dp")
    d.C = d.n_dp // CORES
    d.R = width // d.n_dp
    d.AW = d.R if d.R % LANES == 0 else CORES * d.R
    d.WC = math.gcd(512, d.N)
    d.NB = d.N // d.WC
    d.PQ = 8
    pieces = d.L * d.NB
    tiles = d.R // TILE * (d.WC // LANES)
    rows = d.R * d.L * d.N // LANES
    d.rows_q = rows // d.PQ
    count = d.n_tp * d.n_dp
    hbm = pl.BlockSpec(memory_space=pl.ANY)
    dma = pltpu.SemaphoreType.DMA
    flat = jax.ShapeDtypeStruct((rows, LANES), jnp.float32)
    return pl.pallas_call(
        functools.partial(step_kernel, d),
        out_shape=(flat, flat, flat, jax.ShapeDtypeStruct((d.n_dp * rows, LANES), jnp.bfloat16)),
        in_specs=[hbm] * 5,
        out_specs=[hbm] * 4,
        scratch_shapes=[
            pltpu.VMEM((CORES, d.L, d.C, d.T, d.AW), jnp.bfloat16),
            pltpu.VMEM((CORES, d.L, d.NB, d.T, d.WC), jnp.bfloat16),
            pltpu.VMEM((d.R, d.WC), jnp.float32),
            pltpu.VMEM((2, d.C - 1, pieces, tiles + 1, TILE, LANES), jnp.bfloat16),
            pltpu.VMEM((rows, LANES), jnp.float32),
            pltpu.VMEM((d.C, d.PQ, d.rows_q, LANES), jnp.bfloat16),
            pltpu.VMEM((3, STATE_SLOTS, d.rows_q, LANES), jnp.float32),
            pltpu.VMEM((count, 1, LANES), jnp.float32),
            dma((d.L, d.C)), dma((d.L, d.C)), dma((d.L, d.C)),
            dma((d.L, d.NB)), dma((d.L, d.NB)), dma((d.L, d.NB)),
            dma((2, d.C - 1, pieces)), dma((2, d.C - 1, pieces)),
            dma((count,)), dma((count,)),
            dma((3, STATE_SLOTS)), dma((3, STATE_SLOTS)),
            dma((2, d.C, d.PQ)), dma((d.C, d.PQ)),
            dma((d.C, d.PQ)), dma((d.C, d.PQ)), dma((d.C, d.PQ)),
        ],
        compiler_params=pltpu.CompilerParams(
            collective_id=0, has_side_effects=True, vmem_limit_bytes=67043328
        ),
        name="whole_step",
    )(acts, grads, master, first, second)


def to_rows(x):
    r, l, n = x.shape
    return x.reshape(r, l, n // LANES, LANES).transpose(0, 2, 1, 3).reshape(-1, LANES)


def from_rows(y, l, n):
    return y.reshape(-1, n // LANES, l, LANES).transpose(0, 2, 1, 3).reshape(-1, l, n)


def on_device(activations, out_grads, master, first_moment, second_moment):
    states = [to_rows(x) for x in (master, first_moment, second_moment)]
    outs = whole_step(activations, out_grads, *states)
    return tuple(from_rows(y, *master.shape[1:]) for y in outs)


def solution(mesh):
    return jax.shard_map(
        on_device,
        mesh=mesh,
        in_specs=(
            P(None, "dp", "tp"),
            P(None, "dp", None),
            P(("tp", "dp"), None, None),
            P(("tp", "dp"), None, None),
            P(("tp", "dp"), None, None),
        ),
        out_specs=(
            P(("tp", "dp"), None, None),
            P(("tp", "dp"), None, None),
            P(("tp", "dp"), None, None),
            P("tp", None, None),
        ),
        check_vma=False,
    )
```

```python
import functools
import math

import jax
import jax.numpy as jnp
from jax import lax
from jax.experimental import pallas as pl
from jax.experimental.pallas import tpu as pltpu
from jax.sharding import PartitionSpec as P

beta_first = 0.9
beta_second = 0.95
first_fix = 1.0 - 0.9**10
second_fix = 1.0 - 0.95**10
learn_rate = 0.01
decay_rate = 0.1
epsilon = 1e-08
limit_scale = 2.0
MESH = pl.DeviceIdType.MESH
CORES = 2
LANES = 128
TILE = 16
TOP = 224.0
STATE_SLOTS = 4
LAG = 2


def decode(code, scale):
    code = code.astype(jnp.float32)
    size = jnp.abs(code)
    root = jnp.exp(jnp.log(jnp.maximum(size, 1e-37)) * (1.0 / 16.0))
    root = jnp.where(size > 0.0, root, 0.0)
    return jnp.where(code < 0.0, -root, root) * scale


def encode(value, shrink):
    x = value * shrink
    power = x * x
    power = power * power
    power = power * power
    power = power * power
    return jnp.where(x < 0.0, -power, power).astype(jnp.bfloat16)


def step_kernel(
    d,
    acts, grads, master, first, second,
    new_master, new_first, new_second, weights,
    a_buf, b_buf, part, rx, grad, wide, state, norm,
    a_own, a_send, a_recv, b_own, b_send, b_recv,
    rs_send, rs_recv, norm_send, norm_recv, state_in, state_out,
    ag_send, ag_recv, out_local, out_send, out_recv,
):
    L, T, R, N, C, AW, WC, NB = d.L, d.T, d.R, d.N, d.C, d.AW, d.WC, d.NB
    n_tp, n_dp = d.n_tp, d.n_dp
    pieces, tiles_across, lane_tiles = L * NB, WC // LANES, N // LANES
    tiles = R // TILE * tiles_across
    stride = lane_tiles * L
    index = lax.axis_index("dp")
    chip, core = index // CORES, lax.rem(index, CORES)
    partner = {"dp": chip * CORES + 1 - core}
    me = lax.axis_index("tp") * n_dp + index
    count = n_tp * n_dp

    def column(c, k):
        start = c * CORES * R + (k * R if AW == R else 0)
        return pl.ds(pl.multiple_of(start, LANES), AW)

    def a_local(l, c):
        return pltpu.make_async_copy(
            acts.at[l, :, column(c, core)], a_buf.at[0, l, c], a_own.at[l, c]
        )

    def a_remote(l, c):
        return pltpu.make_async_remote_copy(
            acts.at[l, :, column(c, 1 - core)], a_buf.at[1, l, c],
            a_send.at[l, c], a_recv.at[l, c],
            device_id=partner, device_id_type=MESH,
        )

    def b_columns(j):
        return pl.ds(pl.multiple_of(j * WC, LANES), WC)

    def b_local(l, j):
        return pltpu.make_async_copy(
            grads.at[l, :, b_columns(j)], b_buf.at[0, l, j], b_own.at[l, j]
        )

    def b_remote(l, j):
        return pltpu.make_async_remote_copy(
            grads.at[l, :, b_columns(j)], b_buf.at[1, l, j],
            b_send.at[l, j], b_recv.at[l, j],
            device_id=partner, device_id_type=MESH,
        )

    def in_order(a_copy, b_copy):
        for l in range(L):
            a_copy(l, C - 1).start()
            a_copy(l, 0).start()
            for j in range(NB):
                b_copy(l, j).start()
            for c in range(1, C - 1):
                a_copy(l, c).start()

    in_order(a_local, b_local)

    rows_q = d.rows_q
    sources = (master, first, second)
    targets = (new_master, new_first, new_second)

    def state_load(i, q):
        slot = lax.rem(q, STATE_SLOTS)
        return pltpu.make_async_copy(
            sources[i].at[pl.ds(q * rows_q, rows_q)], state.at[i, slot], state_in.at[i, slot]
        )

    def state_store(i, q):
        slot = lax.rem(q, STATE_SLOTS)
        return pltpu.make_async_copy(
            state.at[i, slot], targets[i].at[pl.ds(q * rows_q, rows_q)], state_out.at[i, slot]
        )

    barrier = pltpu.get_barrier_semaphore()

    def device(k):
        other = lax.rem(me + k, count)
        return {"tp": other // n_dp, "dp": lax.rem(other, n_dp)}

    @pl.loop(1, count)
    def _(k):
        pl.semaphore_signal(barrier, inc=1, device_id=device(k), device_id_type=MESH)

    pl.semaphore_wait(barrier, count - 1)

    in_order(a_remote, b_remote)

    for q in range(min(STATE_SLOTS, d.PQ)):
        for i in range(3):
            state_load(i, jnp.int32(q)).start()

    def product(c, l, j):
        total = None
        for w in range(CORES):
            lhs = a_buf[w, l, c]
            if AW != R:
                lhs = jnp.where(core == 0, lhs[:, :R], lhs[:, R:])
            term = lax.dot_general(
                lhs, b_buf[w, l, j], (((0,), (0,)), ((), ())),
                preferred_element_type=jnp.float32,
            )
            total = term if total is None else total + term
        part[...] = total

    def rs_copy(way, s, p):
        to = chip + 1 if way == 0 else chip - 1
        return pltpu.make_async_remote_copy(
            rx.at[way, s, p], rx.at[way, s, p],
            rs_send.at[way, s, p], rs_recv.at[way, s, p],
            device_id={"dp": to * CORES + core}, device_id_type=MESH,
        )

    def add_received(way, s, p):
        rs_copy(way, s, p).wait_recv()
        scale = rx[way, s, p, tiles].astype(jnp.float32) * (1.0 / TOP)

        @pl.loop(0, R // TILE)
        def _(r):
            rows = pl.ds(pl.multiple_of(r * TILE, TILE), TILE)
            for t in range(tiles_across):
                lanes = pl.ds(t * LANES, LANES)
                code = rx[way, s, p, r * tiles_across + t]
                part[rows, lanes] += decode(code, scale)

    def send_on(way, s, p):
        def widest(r, top):
            rows = pl.ds(pl.multiple_of(r * TILE, TILE), TILE)
            for t in range(tiles_across):
                top = jnp.maximum(top, jnp.abs(part[rows, pl.ds(t * LANES, LANES)]))
            return top

        top = lax.fori_loop(0, R // TILE, widest, jnp.zeros((TILE, LANES), jnp.float32))
        top = jnp.maximum(top, 1e-25).astype(jnp.bfloat16)
        rx[way, s, p, tiles] = top
        shrink = TOP / top.astype(jnp.float32)

        @pl.loop(0, R // TILE)
        def _(r):
            rows = pl.ds(pl.multiple_of(r * TILE, TILE), TILE)
            for t in range(tiles_across):
                value = part[rows, pl.ds(t * LANES, LANES)]
                rx[way, s, p, r * tiles_across + t] = encode(value, shrink)

        rs_copy(way, s, p).start()

    def own_rows(r, l, j, t, half):
        start = ((r * TILE + half * 8) * lane_tiles + j * tiles_across + t) * L + l
        return pl.ds(start, 8, stride=stride)

    def keep_own(l, j):
        @pl.loop(0, R // TILE)
        def _(r):
            rows = pl.ds(pl.multiple_of(r * TILE, TILE), TILE)
            for t in range(tiles_across):
                value = part[rows, pl.ds(t * LANES, LANES)]
                for half in range(2):
                    grad[own_rows(r, l, j, t, half), :] = value[half * 8 : half * 8 + 8]

    def add_own(way, s, p, l, j):
        rs_copy(way, s, p).wait_recv()
        scale = rx[way, s, p, tiles].astype(jnp.float32) * (1.0 / TOP)

        @pl.loop(0, R // TILE)
        def _(r):
            for t in range(tiles_across):
                value = decode(rx[way, s, p, r * tiles_across + t], scale)
                for half in range(2):
                    where = own_rows(r, l, j, t, half)
                    grad[where, :] = grad[where, :] + value[half * 8 : half * 8 + 8]

    steps = (C - 1) * pieces

    def stream(way, t):
        hops = chip if way == 0 else C - 1 - chip
        n = t - LAG * hops
        s, p = n // pieces, lax.rem(n, pieces)
        owner = C - 1 - s if way == 0 else s
        ahead = chip < owner if way == 0 else chip > owner

        @pl.when((n >= 0) & (n < steps) & ahead)
        def _():
            product(owner, p // NB, lax.rem(p, NB))

            @pl.when(hops > 0)
            def _():
                add_received(way, s, p)

            send_on(way, s, p)

    def arrival(way, t):
        hops = chip if way == 0 else C - 1 - chip
        n = t - LAG * hops - 1
        s, p = n // pieces, lax.rem(n, pieces)
        owner = C - 1 - s if way == 0 else s

        @pl.when((n >= 0) & (n < steps) & (chip == owner) & (hops > 0))
        def _():
            add_own(way, s, p, p // NB, lax.rem(p, NB))

    @pl.loop(0, steps + LAG * (C - 1) + 1)
    def _(t):
        l, j = t // NB, lax.rem(t, NB)

        @pl.when(t < pieces)
        def _():
            @pl.when(j == 0)
            def _():
                for c in sorted({0, C - 1}):
                    a_local(l, c).wait()
                    a_remote(l, c).wait_recv()

            b_local(l, j).wait()
            b_remote(l, j).wait_recv()

        stream(0, t)
        stream(1, t)

        @pl.when(t < pieces)
        def _():
            @pl.when(j == 0)
            def _():
                for c in range(1, C - 1):
                    a_local(l, c).wait()
                    a_remote(l, c).wait_recv()

            product(chip, l, j)
            keep_own(l, j)

        arrival(0, t)
        arrival(1, t)

    own_total = R * stride
    block = 64

    def square(b, sums):
        x = grad[pl.ds(pl.multiple_of(b * block, block), block), :]
        x = x * x
        for i in range(block // 8):
            sums = sums + x[i * 8 : i * 8 + 8]
        return sums

    sums = lax.fori_loop(0, own_total // block, square, jnp.zeros((8, LANES), jnp.float32))
    norm[me] = jnp.sum(sums, axis=0, keepdims=True)

    def norm_copy(k, slot):
        return pltpu.make_async_remote_copy(
            norm.at[slot], norm.at[slot], norm_send.at[k], norm_recv.at[k],
            device_id=device(k), device_id_type=MESH,
        )

    @pl.loop(1, count)
    def _(k):
        norm_copy(k, me).start()

    @pl.loop(1, count)
    def _(k):
        norm_copy(k, lax.rem(me - k + count, count)).wait_recv()

    total = jnp.sum(jnp.sum(norm[...], axis=0), axis=1, keepdims=True)
    limit = limit_scale * math.sqrt(own_total * LANES * count)
    clip = limit / jnp.maximum(jnp.sqrt(total), limit)
    clip = jnp.broadcast_to(clip, (block, LANES))

    def place(c, q):
        start = (c * CORES + core) * own_total + q * rows_q
        return pl.ds(pl.multiple_of(start, TILE), rows_q)

    def ag_copy(way, c, q):
        to = chip + 1 if way == 0 else chip - 1
        return pltpu.make_async_remote_copy(
            wide.at[c, q], wide.at[c, q], ag_send.at[way, c, q], ag_recv.at[c, q],
            device_id={"dp": to * CORES + core}, device_id_type=MESH,
        )

    def local_copy(c, q):
        return pltpu.make_async_copy(wide.at[c, q], weights.at[place(c, q)], out_local.at[c, q])

    def partner_copy(c, q):
        return pltpu.make_async_remote_copy(
            wide.at[c, q], weights.at[place(c, q)], out_send.at[c, q], out_recv.at[c, q],
            device_id=partner, device_id_type=MESH,
        )

    def partner_place(c, q):
        start = (c * CORES + 1 - core) * own_total + q * rows_q
        return pl.ds(pl.multiple_of(start, TILE), rows_q)

    def partner_arrival(c, q):
        return pltpu.make_async_remote_copy(
            wide.at[c, q], weights.at[partner_place(c, q)], out_send.at[c, q], out_recv.at[c, q],
            device_id=partner, device_id_type=MESH,
        )

    @pl.loop(0, d.PQ)
    def _(q):
        slot = lax.rem(q, STATE_SLOTS)
        for i in range(3):
            state_load(i, q).wait()

        @pl.loop(0, rows_q // block)
        def _(b):
            here = pl.ds(pl.multiple_of(b * block, block), block)
            there = pl.ds(pl.multiple_of(q * rows_q + b * block, block), block)
            clipped = clip * grad[there, :]
            moment = beta_first * state[1, slot, here, :] + (1.0 - beta_first) * clipped
            spread = beta_second * state[2, slot, here, :]
            spread = spread + (1.0 - beta_second) * clipped * clipped
            old = state[0, slot, here, :]
            direction = moment / first_fix / (jnp.sqrt(spread / second_fix) + epsilon)
            new = old - learn_rate * (direction + decay_rate * old)
            state[0, slot, here, :] = new
            state[1, slot, here, :] = moment
            state[2, slot, here, :] = spread
            wide[chip, q, here, :] = new.astype(jnp.bfloat16)

        @pl.when(chip > 0)
        def _():
            ag_copy(1, chip, q).start()

        @pl.when(chip < C - 1)
        def _():
            ag_copy(0, chip, q).start()

        for i in range(3):
            state_store(i, q).start()
        local_copy(chip, q).start()
        partner_copy(chip, q).start()

        @pl.when((q > 0) & (q - 1 + STATE_SLOTS < d.PQ))
        def _():
            for i in range(3):
                state_store(i, q - 1).wait()
                state_load(i, q - 1 + STATE_SLOTS).start()

    @pl.loop(1, C)
    def _(far):
        @pl.loop(0, d.PQ)
        def _(q):
            @pl.when(chip - far >= 0)
            def _():
                ag_copy(0, chip - far, q).wait_recv()

                @pl.when(chip < C - 1)
                def _():
                    ag_copy(0, chip - far, q).start()

                local_copy(chip - far, q).start()
                partner_copy(chip - far, q).start()

            @pl.when(chip + far < C)
            def _():
                ag_copy(1, chip + far, q).wait_recv()

                @pl.when(chip > 0)
                def _():
                    ag_copy(1, chip + far, q).start()

                local_copy(chip + far, q).start()
                partner_copy(chip + far, q).start()

    for q in range(max(0, d.PQ - STATE_SLOTS), d.PQ):
        for i in range(3):
            state_store(i, jnp.int32(q)).wait()

    for l in range(L):
        for c in range(C):
            a_remote(l, c).wait_send()
        for j in range(NB):
            b_remote(l, j).wait_send()

    @pl.loop(1, count)
    def _(k):
        norm_copy(k, me).wait_send()

    @pl.loop(0, C - 1)
    def _(s):
        @pl.loop(0, pieces)
        def _(p):
            @pl.when(chip < C - 1 - s)
            def _():
                rs_copy(0, s, p).wait_send()

            @pl.when(chip > s)
            def _():
                rs_copy(1, s, p).wait_send()

    @pl.loop(0, C)
    def _(c):
        @pl.loop(0, d.PQ)
        def _(q):
            @pl.when((c <= chip) & (chip < C - 1))
            def _():
                ag_copy(0, c, q).wait_send()

            @pl.when((c >= chip) & (chip > 0))
            def _():
                ag_copy(1, c, q).wait_send()

            local_copy(c, q).wait()
            partner_copy(c, q).wait_send()
            partner_arrival(c, q).wait_recv()


class Sizes:
    pass


def whole_step(acts, grads, master, first, second):
    d = Sizes()
    d.L, d.T, width = acts.shape
    d.N = grads.shape[2]
    d.n_tp, d.n_dp = lax.axis_size("tp"), lax.axis_size("dp")
    d.C = d.n_dp // CORES
    d.R = width // d.n_dp
    d.AW = d.R if d.R % LANES == 0 else CORES * d.R
    d.WC = math.gcd(512, d.N)
    d.NB = d.N // d.WC
    d.PQ = 8
    pieces = d.L * d.NB
    tiles = d.R // TILE * (d.WC // LANES)
    rows = d.R * d.L * d.N // LANES
    d.rows_q = rows // d.PQ
    count = d.n_tp * d.n_dp
    hbm = pl.BlockSpec(memory_space=pl.ANY)
    dma = pltpu.SemaphoreType.DMA
    flat = jax.ShapeDtypeStruct((rows, LANES), jnp.float32)
    return pl.pallas_call(
        functools.partial(step_kernel, d),
        out_shape=(flat, flat, flat, jax.ShapeDtypeStruct((d.n_dp * rows, LANES), jnp.bfloat16)),
        in_specs=[hbm] * 5,
        out_specs=[hbm] * 4,
        scratch_shapes=[
            pltpu.VMEM((CORES, d.L, d.C, d.T, d.AW), jnp.bfloat16),
            pltpu.VMEM((CORES, d.L, d.NB, d.T, d.WC), jnp.bfloat16),
            pltpu.VMEM((d.R, d.WC), jnp.float32),
            pltpu.VMEM((2, d.C - 1, pieces, tiles + 1, TILE, LANES), jnp.bfloat16),
            pltpu.VMEM((rows, LANES), jnp.float32),
            pltpu.VMEM((d.C, d.PQ, d.rows_q, LANES), jnp.bfloat16),
            pltpu.VMEM((3, STATE_SLOTS, d.rows_q, LANES), jnp.float32),
            pltpu.VMEM((count, 1, LANES), jnp.float32),
            dma((d.L, d.C)), dma((d.L, d.C)), dma((d.L, d.C)),
            dma((d.L, d.NB)), dma((d.L, d.NB)), dma((d.L, d.NB)),
            dma((2, d.C - 1, pieces)), dma((2, d.C - 1, pieces)),
            dma((count,)), dma((count,)),
            dma((3, STATE_SLOTS)), dma((3, STATE_SLOTS)),
            dma((2, d.C, d.PQ)), dma((d.C, d.PQ)),
            dma((d.C, d.PQ)), dma((d.C, d.PQ)), dma((d.C, d.PQ)),
        ],
        compiler_params=pltpu.CompilerParams(
            collective_id=0, has_side_effects=True, vmem_limit_bytes=67043328
        ),
        name="whole_step",
    )(acts, grads, master, first, second)


def to_rows(x):
    r, l, n = x.shape
    return x.reshape(r, l, n // LANES, LANES).transpose(0, 2, 1, 3).reshape(-1, LANES)


def from_rows(y, l, n):
    return y.reshape(-1, n // LANES, l, LANES).transpose(0, 2, 1, 3).reshape(-1, l, n)


def on_device(activations, out_grads, master, first_moment, second_moment):
    states = [to_rows(x) for x in (master, first_moment, second_moment)]
    outs = whole_step(activations, out_grads, *states)
    return tuple(from_rows(y, *master.shape[1:]) for y in outs)


def solution(mesh):
    return jax.shard_map(
        on_device,
        mesh=mesh,
        in_specs=(
            P(None, "dp", "tp"),
            P(None, "dp", None),
            P(("tp", "dp"), None, None),
            P(("tp", "dp"), None, None),
            P(("tp", "dp"), None, None),
        ),
        out_specs=(
            P(("tp", "dp"), None, None),
            P(("tp", "dp"), None, None),
            P(("tp", "dp"), None, None),
            P("tp", None, None),
        ),
        check_vma=False,
    )
```

```python
import functools
import math

import jax
import jax.numpy as jnp
from jax import lax
from jax.experimental import pallas as pl
from jax.experimental.pallas import tpu as pltpu
from jax.sharding import PartitionSpec as P

beta_first = 0.9
beta_second = 0.95
first_fix = 1.0 - 0.9**10
second_fix = 1.0 - 0.95**10
learn_rate = 0.01
decay_rate = 0.1
epsilon = 1e-08
limit_scale = 2.0
MESH = pl.DeviceIdType.MESH
CORES = 2
LANES = 128
TILE = 16
TOP = 224.0
STATE_SLOTS = 4
LAG = 2
SPLIT = 2
BEHIND = 3
FLIGHT = 2


def decode(code, scale):
    code = code.astype(jnp.float32)
    size = jnp.abs(code)
    root = jnp.exp(jnp.log(jnp.maximum(size, 1e-37)) * (1.0 / 16.0))
    root = jnp.where(size > 0.0, root, 0.0)
    return jnp.where(code < 0.0, -root, root) * scale


def encode(value, shrink):
    x = value * shrink
    power = x * x
    power = power * power
    power = power * power
    power = power * power
    return jnp.where(x < 0.0, -power, power).astype(jnp.bfloat16)


def step_kernel(
    d,
    acts, grads, master, first, second,
    new_master, new_first, new_second, weights,
    a_buf, b_buf, part, rx, tot, grad, wide, state, squares, norm,
    a_own, a_send, a_recv, b_own, b_send, b_recv,
    rs_send, rs_recv, tot_send, tot_recv, norm_send, norm_recv, state_in, state_out,
    ag_send, ag_recv, out_local, out_send, out_recv,
):
    L, T, R, N, C, AW, WC, NB = d.L, d.T, d.R, d.N, d.C, d.AW, d.WC, d.NB
    n_tp, n_dp = d.n_tp, d.n_dp
    pieces, tiles_across, lane_tiles = L * NB, WC // LANES, N // LANES
    tiles = R // TILE * tiles_across
    group = tiles_across * L
    half, rows_u = C // 2, R // SPLIT
    index = lax.axis_index("dp")
    chip, core = index // CORES, lax.rem(index, CORES)
    partner = {"dp": chip * CORES + 1 - core}
    me = lax.axis_index("tp") * n_dp + index
    count = n_tp * n_dp

    def column(c, k):
        start = c * CORES * R + (k * R if AW == R else 0)
        return pl.ds(pl.multiple_of(start, LANES), AW)

    def a_local(l, c):
        return pltpu.make_async_copy(
            acts.at[l, :, column(c, core)], a_buf.at[0, l, c], a_own.at[l, c]
        )

    def a_remote(l, c):
        return pltpu.make_async_remote_copy(
            acts.at[l, :, column(c, 1 - core)], a_buf.at[1, l, c],
            a_send.at[l, c], a_recv.at[l, c],
            device_id=partner, device_id_type=MESH,
        )

    def b_columns(j):
        return pl.ds(pl.multiple_of(j * WC, LANES), WC)

    def b_local(l, j):
        return pltpu.make_async_copy(
            grads.at[l, :, b_columns(j)], b_buf.at[0, l, j], b_own.at[l, j]
        )

    def b_remote(l, j):
        return pltpu.make_async_remote_copy(
            grads.at[l, :, b_columns(j)], b_buf.at[1, l, j],
            b_send.at[l, j], b_recv.at[l, j],
            device_id=partner, device_id_type=MESH,
        )

    def in_order(a_copy, b_copy):
        for l in range(L):
            for c in sorted({half - 1, half}):
                a_copy(l, c).start()
        for j in range(NB):
            for l in range(L):
                b_copy(l, j).start()
        for c in range(C):
            if c not in (half - 1, half):
                for l in range(L):
                    a_copy(l, c).start()

    in_order(a_local, b_local)

    sources = (master, first, second)
    targets = (new_master, new_first, new_second)

    def unit(start, q):
        rows = start + lax.rem(q, SPLIT) * rows_u
        return (
            pl.ds(pl.multiple_of(rows, TILE), rows_u),
            pl.ds(pl.multiple_of(q // SPLIT * group, group), group),
        )

    def state_load(i, q):
        slot = lax.rem(q, STATE_SLOTS)
        return pltpu.make_async_copy(
            sources[i].at[unit(0, q)], state.at[i, slot], state_in.at[i, slot]
        )

    def state_store(i, q):
        slot = lax.rem(q, STATE_SLOTS)
        return pltpu.make_async_copy(
            state.at[i, slot], targets[i].at[unit(0, q)], state_out.at[i, slot]
        )

    barrier = pltpu.get_barrier_semaphore()

    def device(k):
        other = lax.rem(me + k, count)
        return {"tp": other // n_dp, "dp": lax.rem(other, n_dp)}

    @pl.loop(1, count)
    def _(k):
        pl.semaphore_signal(barrier, inc=1, device_id=device(k), device_id_type=MESH)

    pl.semaphore_wait(barrier, count - 1)

    in_order(a_remote, b_remote)

    for q in range(min(STATE_SLOTS, d.PQ)):
        for i in range(3):
            state_load(i, jnp.int32(q)).start()

    def product(c, l, j):
        total = None
        for w in range(CORES):
            lhs = a_buf[w, l, c]
            if AW != R:
                lhs = jnp.where(core == 0, lhs[:, :R], lhs[:, R:])
            term = lax.dot_general(
                lhs, b_buf[w, l, j], (((0,), (0,)), ((), ())),
                preferred_element_type=jnp.float32,
            )
            total = term if total is None else total + term
        part[...] = total

    def rs_copy(way, s, p):
        to = chip + 1 if way == 0 else chip - 1
        return pltpu.make_async_remote_copy(
            rx.at[way, s, p], rx.at[way, s, p],
            rs_send.at[way, s, p], rs_recv.at[way, s, p],
            device_id={"dp": to * CORES + core}, device_id_type=MESH,
        )

    def add_received(way, s, p):
        rs_copy(way, s, p).wait_recv()
        scale = rx[way, s, p, tiles].astype(jnp.float32) * (1.0 / TOP)

        @pl.loop(0, R // TILE)
        def _(r):
            rows = pl.ds(pl.multiple_of(r * TILE, TILE), TILE)
            for t in range(tiles_across):
                lanes = pl.ds(t * LANES, LANES)
                code = rx[way, s, p, r * tiles_across + t]
                part[rows, lanes] += decode(code, scale)

    def pack(way, s, p):
        def widest(r, top):
            rows = pl.ds(pl.multiple_of(r * TILE, TILE), TILE)
            for t in range(tiles_across):
                top = jnp.maximum(top, jnp.abs(part[rows, pl.ds(t * LANES, LANES)]))
            return top

        top = lax.fori_loop(0, R // TILE, widest, jnp.zeros((TILE, LANES), jnp.float32))
        top = jnp.maximum(top, 1e-25).astype(jnp.bfloat16)
        rx[way, s, p, tiles] = top
        shrink = TOP / top.astype(jnp.float32)

        @pl.loop(0, R // TILE)
        def _(r):
            rows = pl.ds(pl.multiple_of(r * TILE, TILE), TILE)
            for t in range(tiles_across):
                value = part[rows, pl.ds(t * LANES, LANES)]
                rx[way, s, p, r * tiles_across + t] = encode(value, shrink)

    def put(r, l, j, t, value):
        for k in range(TILE // 8):
            start = (j * R + r * TILE + k * 8) * group + t * L + l
            grad[pl.ds(start, 8, stride=group), :] = value[k * 8 : k * 8 + 8]

    def keep_part(l, j):
        @pl.loop(0, R // TILE)
        def _(r):
            rows = pl.ds(pl.multiple_of(r * TILE, TILE), TILE)
            for t in range(tiles_across):
                put(r, l, j, t, part[rows, pl.ds(t * LANES, LANES)])

    def add_squares():
        def square(r, sums):
            rows = pl.ds(pl.multiple_of(r * TILE, TILE), TILE)
            for t in range(tiles_across):
                x = part[rows, pl.ds(t * LANES, LANES)]
                sums = sums + x * x
            return sums

        squares[...] = lax.fori_loop(0, R // TILE, square, squares[...])

    def owner_of(way, s):
        return half + s if way == 0 else half - 1 - s

    def tot_copy(way, s, p):
        return pltpu.make_async_remote_copy(
            rx.at[way, s, p], tot.at[p], tot_send.at[s, p], tot_recv.at[p],
            device_id={"dp": owner_of(way, s) * CORES + core}, device_id_type=MESH,
        )

    steps = half * pieces
    squares[...] = jnp.zeros_like(squares)

    def stream(way, t):
        hops = chip if way == 0 else C - 1 - chip
        n = t - LAG * hops
        s, p = n // pieces, lax.rem(n, pieces)
        l, j = lax.rem(p, L), p // L

        @pl.when((n >= 0) & (n < steps))
        def _():
            product(owner_of(way, s), l, j)

            @pl.when(hops > 0)
            def _():
                add_received(way, s, p)

            @pl.when(hops == C - 1)
            def _():
                add_squares()

            last = (hops == C - 1) & (s == half - 1)

            @pl.when(last)
            def _():
                keep_part(l, j)

            @pl.when(jnp.logical_not(last))
            def _():
                pack(way, s, p)

            @pl.when((hops < C - 1) & (n >= FLIGHT))
            def _():
                before = n - FLIGHT
                rs_copy(way, before // pieces, lax.rem(before, pieces)).wait_send()

            @pl.when(hops < C - 1)
            def _():
                rs_copy(way, s, p).start()

    totals = (half - 1) * pieces
    leave = max(steps, totals + LAG * (C - 1))
    in_loop = min(totals, steps + LAG * (C - 1) - leave)

    def at_sink(way):
        return chip == (C - 1 if way == 0 else 0)

    def send_total(n):
        for way in range(2):
            @pl.when(at_sink(way))
            def _():
                @pl.when(n >= FLIGHT)
                def _():
                    before = n - FLIGHT
                    tot_copy(way, before // pieces, lax.rem(before, pieces)).wait_send()

                tot_copy(way, n // pieces, lax.rem(n, pieces)).start()

    @pl.loop(0, steps + LAG * (C - 1))
    def _(t):
        l, j = lax.rem(t, L), t // L

        @pl.when(t < pieces)
        def _():
            @pl.when(j == 0)
            def _():
                for c in sorted({half - 1, half}):
                    a_local(l, c).wait()
                    a_remote(l, c).wait_recv()

            b_local(l, j).wait()
            b_remote(l, j).wait_recv()

        @pl.when((t >= pieces) & (t < pieces + L))
        def _():
            for c in range(C):
                if c not in (half - 1, half):
                    a_local(t - pieces, c).wait()
                    a_remote(t - pieces, c).wait_recv()

        stream(0, t)
        stream(1, t)

        @pl.when((t >= leave) & (t < leave + in_loop))
        def _():
            send_total(t - leave)

    norm[me] = jnp.sum(squares[...], axis=0, keepdims=True)

    def norm_copy(k, slot):
        return pltpu.make_async_remote_copy(
            norm.at[slot], norm.at[slot], norm_send.at[k], norm_recv.at[k],
            device_id=device(k), device_id_type=MESH,
        )

    at_end = (chip == 0) | (chip == C - 1)

    def from_end(k):
        other = lax.rem(lax.rem(me - k + count, count), n_dp) // CORES
        return (other == 0) | (other == C - 1)

    @pl.when(at_end)
    def _():
        @pl.loop(1, count)
        def _(k):
            norm_copy(k, me).start()

    @pl.loop(1, count)
    def _(k):
        @pl.when(from_end(k))
        def _():
            norm_copy(k, lax.rem(me - k + count, count)).wait_recv()

    @pl.loop(in_loop, totals)
    def _(n):
        send_total(n)

    total = None
    for a in range(n_tp):
        for c in sorted({0, C - 1}):
            for k in range(CORES):
                row = norm[a * n_dp + c * CORES + k]
                total = row if total is None else total + row
    total = jnp.sum(total, axis=1, keepdims=True)
    limit = limit_scale * math.sqrt(R * L * N * count)
    clip = limit / jnp.maximum(jnp.sqrt(total), limit)
    block = 8
    clip = jnp.broadcast_to(clip, (block * group, LANES))

    def place(c, q):
        return unit((c * CORES + core) * R, q)

    def ag_copy(way, c, q):
        to = chip + 1 if way == 0 else chip - 1
        return pltpu.make_async_remote_copy(
            wide.at[c, q], wide.at[c, q], ag_send.at[way, c, q], ag_recv.at[c, q],
            device_id={"dp": to * CORES + core}, device_id_type=MESH,
        )

    def local_copy(c, q):
        return pltpu.make_async_copy(wide.at[c, q], weights.at[place(c, q)], out_local.at[c, q])

    def partner_copy(c, q):
        return pltpu.make_async_remote_copy(
            wide.at[c, q], weights.at[place(c, q)], out_send.at[c, q], out_recv.at[c, q],
            device_id=partner, device_id_type=MESH,
        )

    def partner_place(c, q):
        return unit((c * CORES + 1 - core) * R, q)

    def partner_arrival(c, q):
        return pltpu.make_async_remote_copy(
            wide.at[c, q], weights.at[partner_place(c, q)], out_send.at[c, q], out_recv.at[c, q],
            device_id=partner, device_id_type=MESH,
        )

    def update(q):
        slot, j = lax.rem(q, STATE_SLOTS), q // SPLIT

        @pl.when(jnp.logical_not(at_end) & (lax.rem(q, SPLIT) == 0))
        def _():
            for l in range(L):
                p = j * L + l
                tot_copy(0, 0, p).wait_recv()
                scale = tot[p, tiles].astype(jnp.float32) * (1.0 / TOP)

                @pl.loop(0, R // TILE)
                def _(r):
                    for t in range(tiles_across):
                        put(r, l, j, t, decode(tot[p, r * tiles_across + t], scale))

        for i in range(3):
            state_load(i, q).wait()

        @pl.loop(0, rows_u // block)
        def _(b):
            here = pl.ds(pl.multiple_of(b * block, block), block)
            start = (j * R + lax.rem(q, SPLIT) * rows_u + b * block) * group
            there = pl.ds(pl.multiple_of(start, block * group), block * group)

            def read(i):
                return state[i, slot, here].reshape(block * group, LANES)

            def write(i, value):
                state[i, slot, here] = value.reshape(block, group, LANES)

            clipped = clip * grad[there, :]
            moment = beta_first * read(1) + (1.0 - beta_first) * clipped
            spread = beta_second * read(2) + (1.0 - beta_second) * clipped * clipped
            old = read(0)
            direction = moment / first_fix / (jnp.sqrt(spread / second_fix) + epsilon)
            new = old - learn_rate * (direction + decay_rate * old)
            write(0, new)
            write(1, moment)
            write(2, spread)
            wide[chip, q, here] = new.astype(jnp.bfloat16).reshape(block, group, LANES)

        @pl.when(chip > 0)
        def _():
            ag_copy(1, chip, q).start()

        @pl.when(chip < C - 1)
        def _():
            ag_copy(0, chip, q).start()

        for i in range(3):
            state_store(i, q).start()
        local_copy(chip, q).start()
        partner_copy(chip, q).start()

        @pl.when((q > 0) & (q - 1 + STATE_SLOTS < d.PQ))
        def _():
            for i in range(3):
                state_store(i, q - 1).wait()
                state_load(i, q - 1 + STATE_SLOTS).start()

    def pass_on(way, c, q):
        ag_copy(way, c, q).wait_recv()

        @pl.when(chip < C - 1 if way == 0 else chip > 0)
        def _():
            ag_copy(way, c, q).start()

        local_copy(c, q).start()
        partner_copy(c, q).start()

    def relay(way, t):
        room = chip if way == 0 else C - 1 - chip
        chunk, q = (t - BEHIND) // (d.PQ + BEHIND), lax.rem(t - BEHIND, d.PQ + BEHIND)
        near = chip - 1 - chunk if way == 0 else chip + 1 + chunk

        @pl.when((t >= BEHIND) & (chunk < room - 1) & (q < d.PQ))
        def _():
            pass_on(way, near, q)

        late = t - jnp.maximum(room - 1, half - 1) * d.PQ - BEHIND * room

        @pl.when((room > 0) & (late >= 0) & (late < d.PQ))
        def _():
            pass_on(way, 0 if way == 0 else C - 1, late)

    @pl.loop(0, (C - 1) * (d.PQ + BEHIND))
    def _(u):
        @pl.when(u < d.PQ)
        def _():
            update(u)

        relay(0, u)
        relay(1, u)

    for q in range(max(0, d.PQ - STATE_SLOTS), d.PQ):
        for i in range(3):
            state_store(i, jnp.int32(q)).wait()

    for l in range(L):
        for c in range(C):
            a_remote(l, c).wait_send()
        for j in range(NB):
            b_remote(l, j).wait_send()

    @pl.when(at_end)
    def _():
        @pl.loop(1, count)
        def _(k):
            norm_copy(k, me).wait_send()

    @pl.loop(steps - min(FLIGHT, steps), steps)
    def _(n):
        @pl.when(chip < C - 1)
        def _():
            rs_copy(0, n // pieces, lax.rem(n, pieces)).wait_send()

        @pl.when(chip > 0)
        def _():
            rs_copy(1, n // pieces, lax.rem(n, pieces)).wait_send()

    @pl.loop(totals - min(FLIGHT, totals), totals)
    def _(n):
        for way in range(2):
            @pl.when(at_sink(way))
            def _():
                tot_copy(way, n // pieces, lax.rem(n, pieces)).wait_send()

    @pl.loop(0, C)
    def _(c):
        @pl.loop(0, d.PQ)
        def _(q):
            @pl.when((c <= chip) & (chip < C - 1))
            def _():
                ag_copy(0, c, q).wait_send()

            @pl.when((c >= chip) & (chip > 0))
            def _():
                ag_copy(1, c, q).wait_send()

            local_copy(c, q).wait()
            partner_copy(c, q).wait_send()
            partner_arrival(c, q).wait_recv()


class Sizes:
    pass


def whole_step(acts, grads, master, first, second):
    d = Sizes()
    d.L, d.T, width = acts.shape
    d.N = grads.shape[2]
    d.n_tp, d.n_dp = lax.axis_size("tp"), lax.axis_size("dp")
    d.C = d.n_dp // CORES
    d.R = width // d.n_dp
    d.AW = d.R if d.R % LANES == 0 else CORES * d.R
    d.WC = math.gcd(512, d.N)
    d.NB = d.N // d.WC
    d.PQ = d.NB * SPLIT
    pieces = d.L * d.NB
    tiles = d.R // TILE * (d.WC // LANES)
    across = d.L * d.N // LANES
    group = d.L * d.WC // LANES
    count = d.n_tp * d.n_dp
    half = d.C // 2
    packed = (tiles + 1, TILE, LANES)
    hbm = pl.BlockSpec(memory_space=pl.ANY)
    dma = pltpu.SemaphoreType.DMA
    flat = jax.ShapeDtypeStruct((d.R, across, LANES), jnp.float32)
    return pl.pallas_call(
        functools.partial(step_kernel, d),
        out_shape=(flat, flat, flat, jax.ShapeDtypeStruct((d.n_dp * d.R, across, LANES), jnp.bfloat16)),
        in_specs=[hbm] * 5,
        out_specs=[hbm] * 4,
        scratch_shapes=[
            pltpu.VMEM((CORES, d.L, d.C, d.T, d.AW), jnp.bfloat16),
            pltpu.VMEM((CORES, d.L, d.NB, d.T, d.WC), jnp.bfloat16),
            pltpu.VMEM((d.R, d.WC), jnp.float32),
            pltpu.VMEM((2, half, pieces) + packed, jnp.bfloat16),
            pltpu.VMEM((pieces,) + packed, jnp.bfloat16),
            pltpu.VMEM((d.NB * d.R * group, LANES), jnp.float32),
            pltpu.VMEM((d.C, d.PQ, d.R // SPLIT, group, LANES), jnp.bfloat16),
            pltpu.VMEM((3, STATE_SLOTS, d.R // SPLIT, group, LANES), jnp.float32),
            pltpu.VMEM((TILE, LANES), jnp.float32),
            pltpu.VMEM((count, 1, LANES), jnp.float32),
            dma((d.L, d.C)), dma((d.L, d.C)), dma((d.L, d.C)),
            dma((d.L, d.NB)), dma((d.L, d.NB)), dma((d.L, d.NB)),
            dma((2, half, pieces)), dma((2, half, pieces)),
            dma((half, pieces)), dma((pieces,)),
            dma((count,)), dma((count,)),
            dma((3, STATE_SLOTS)), dma((3, STATE_SLOTS)),
            dma((2, d.C, d.PQ)), dma((d.C, d.PQ)),
            dma((d.C, d.PQ)), dma((d.C, d.PQ)), dma((d.C, d.PQ)),
        ],
        compiler_params=pltpu.CompilerParams(
            collective_id=0, has_side_effects=True, vmem_limit_bytes=67043328
        ),
        name="whole_step",
    )(acts, grads, master, first, second)


def to_rows(x):
    r, l, n = x.shape
    return x.reshape(r, l, n // LANES, LANES).transpose(0, 2, 1, 3).reshape(r, -1, LANES)


def from_rows(y, l, n):
    return y.reshape(-1, n // LANES, l, LANES).transpose(0, 2, 1, 3).reshape(-1, l, n)


def on_device(activations, out_grads, master, first_moment, second_moment):
    states = [to_rows(x) for x in (master, first_moment, second_moment)]
    outs = whole_step(activations, out_grads, *states)
    return tuple(from_rows(y, *master.shape[1:]) for y in outs)


def solution(mesh):
    return jax.shard_map(
        on_device,
        mesh=mesh,
        in_specs=(
            P(None, "dp", "tp"),
            P(None, "dp", None),
            P(("tp", "dp"), None, None),
            P(("tp", "dp"), None, None),
            P(("tp", "dp"), None, None),
        ),
        out_specs=(
            P(("tp", "dp"), None, None),
            P(("tp", "dp"), None, None),
            P(("tp", "dp"), None, None),
            P("tp", None, None),
        ),
        check_vma=False,
    )
```

```python
import functools
import math

import jax
import jax.numpy as jnp
from jax import lax
from jax.experimental import pallas as pl
from jax.experimental.pallas import tpu as pltpu
from jax.sharding import PartitionSpec as P

beta_first = 0.9
beta_second = 0.95
first_fix = 1.0 - 0.9**10
second_fix = 1.0 - 0.95**10
learn_rate = 0.01
decay_rate = 0.1
epsilon = 1e-08
limit_scale = 2.0
MESH = pl.DeviceIdType.MESH
CORES = 2
LANES = 128
TILE = 16
TOP = 224.0
STATE_SLOTS = 4
LAG = 2
SPLIT = 2
BEHIND = 3
EARLY, MIDDLE = 3, 3
FLIGHT = 2


def decode(code, scale):
    code = code.astype(jnp.float32)
    size = jnp.abs(code)
    root = jnp.exp(jnp.log(jnp.maximum(size, 1e-37)) * (1.0 / 16.0))
    root = jnp.where(size > 0.0, root, 0.0)
    return jnp.where(code < 0.0, -root, root) * scale


def encode(value, shrink):
    x = value * shrink
    power = x * x
    power = power * power
    power = power * power
    power = power * power
    return jnp.where(x < 0.0, -power, power).astype(jnp.bfloat16)


def step_kernel(
    d,
    acts, grads, master, first, second,
    new_master, new_first, new_second, weights,
    a_buf, b_buf, part, rx, tot, grad, wide, state, squares, norm,
    a_own, a_send, a_recv, b_own, b_send, b_recv,
    rs_send, rs_recv, tot_send, tot_recv, norm_send, norm_recv, state_in, state_out,
    ag_send, ag_recv, out_local, out_send, out_recv,
):
    L, T, R, N, C, AW, WC, NB = d.L, d.T, d.R, d.N, d.C, d.AW, d.WC, d.NB
    n_tp, n_dp = d.n_tp, d.n_dp
    SP, RP = d.SP, d.RP
    pieces, tiles_across, lane_tiles = L * NB * SP, WC // LANES, N // LANES
    tiles = RP // TILE * tiles_across
    group = tiles_across * L
    half, rows_u = C // 2, R // SPLIT
    index = lax.axis_index("dp")
    chip, core = index // CORES, lax.rem(index, CORES)
    partner = {"dp": chip * CORES + 1 - core}
    me = lax.axis_index("tp") * n_dp + index
    count = n_tp * n_dp

    def column(c, k):
        start = c * CORES * R + (k * R if AW == R else 0)
        return pl.ds(pl.multiple_of(start, LANES), AW)

    def a_local(l, c):
        return pltpu.make_async_copy(
            acts.at[l, :, column(c, core)], a_buf.at[0, l, c], a_own.at[l, c]
        )

    def a_remote(l, c):
        return pltpu.make_async_remote_copy(
            acts.at[l, :, column(c, 1 - core)], a_buf.at[1, l, c],
            a_send.at[l, c], a_recv.at[l, c],
            device_id=partner, device_id_type=MESH,
        )

    def b_columns(j):
        return pl.ds(pl.multiple_of(j * WC, LANES), WC)

    def b_local(l, j):
        return pltpu.make_async_copy(
            grads.at[l, :, b_columns(j)], b_buf.at[0, l, j], b_own.at[l, j]
        )

    def b_remote(l, j):
        return pltpu.make_async_remote_copy(
            grads.at[l, :, b_columns(j)], b_buf.at[1, l, j],
            b_send.at[l, j], b_recv.at[l, j],
            device_id=partner, device_id_type=MESH,
        )

    def in_order(a_copy, b_copy):
        for l in range(L):
            for c in sorted({half - 1, half}):
                a_copy(l, c).start()
        for j in range(NB):
            for l in range(L):
                b_copy(l, j).start()
        for c in range(C):
            if c not in (half - 1, half):
                for l in range(L):
                    a_copy(l, c).start()

    in_order(a_local, b_local)

    sources = (master, first, second)
    targets = (new_master, new_first, new_second)

    def unit(start, q):
        rows = start + lax.rem(q, SPLIT) * rows_u
        return (
            pl.ds(pl.multiple_of(rows, TILE), rows_u),
            pl.ds(pl.multiple_of(q // SPLIT * group, group), group),
        )

    def state_load(i, q):
        slot = lax.rem(q, STATE_SLOTS)
        return pltpu.make_async_copy(
            sources[i].at[unit(0, q)], state.at[i, slot], state_in.at[i, slot]
        )

    def state_store(i, q):
        slot = lax.rem(q, STATE_SLOTS)
        return pltpu.make_async_copy(
            state.at[i, slot], targets[i].at[unit(0, q)], state_out.at[i, slot]
        )

    barrier = pltpu.get_barrier_semaphore()

    def device(k):
        other = lax.rem(me + k, count)
        return {"tp": other // n_dp, "dp": lax.rem(other, n_dp)}

    @pl.loop(1, count)
    def _(k):
        pl.semaphore_signal(barrier, inc=1, device_id=device(k), device_id_type=MESH)

    pl.semaphore_wait(barrier, count - 1)

    in_order(a_remote, b_remote)

    for q in range(min(STATE_SLOTS, d.PQ)):
        for i in range(3):
            state_load(i, jnp.int32(q)).start()

    def parts_of(p):
        return lax.rem(p, L), p // (L * SP), lax.rem(p // L, SP)

    def product(c, l, j, h):
        total = None
        for w in range(CORES):
            if SP == 1:
                lhs = a_buf[w, l, c]
            else:
                lhs = a_buf[w, l, c, :, pl.ds(pl.multiple_of(h * RP, LANES), RP)]
            if AW != R:
                lhs = jnp.where(core == 0, lhs[:, :R], lhs[:, R:])
            term = lax.dot_general(
                lhs, b_buf[w, l, j], (((0,), (0,)), ((), ())),
                preferred_element_type=jnp.float32,
            )
            total = term if total is None else total + term
        part[...] = total

    def rs_copy(way, s, p):
        to = chip + 1 if way == 0 else chip - 1
        return pltpu.make_async_remote_copy(
            rx.at[way, s, p], rx.at[way, s, p],
            rs_send.at[way, s, p], rs_recv.at[way, s, p],
            device_id={"dp": to * CORES + core}, device_id_type=MESH,
        )

    def add_received(way, s, p):
        rs_copy(way, s, p).wait_recv()
        scale = rx[way, s, p, tiles].astype(jnp.float32) * (1.0 / TOP)

        @pl.loop(0, RP // TILE)
        def _(r):
            rows = pl.ds(pl.multiple_of(r * TILE, TILE), TILE)
            for t in range(tiles_across):
                lanes = pl.ds(t * LANES, LANES)
                code = rx[way, s, p, r * tiles_across + t]
                part[rows, lanes] += decode(code, scale)

    def pack(way, s, p):
        def widest(r, top):
            rows = pl.ds(pl.multiple_of(r * TILE, TILE), TILE)
            for t in range(tiles_across):
                top = jnp.maximum(top, jnp.abs(part[rows, pl.ds(t * LANES, LANES)]))
            return top

        top = lax.fori_loop(0, RP // TILE, widest, jnp.zeros((TILE, LANES), jnp.float32))
        top = jnp.maximum(top, 1e-25).astype(jnp.bfloat16)
        rx[way, s, p, tiles] = top
        shrink = TOP / top.astype(jnp.float32)

        @pl.loop(0, RP // TILE)
        def _(r):
            rows = pl.ds(pl.multiple_of(r * TILE, TILE), TILE)
            for t in range(tiles_across):
                value = part[rows, pl.ds(t * LANES, LANES)]
                rx[way, s, p, r * tiles_across + t] = encode(value, shrink)

    def put(r, l, j, h, t, value):
        for k in range(TILE // 8):
            start = (j * R + h * RP + r * TILE + k * 8) * group + t * L + l
            grad[pl.ds(start, 8, stride=group), :] = value[k * 8 : k * 8 + 8]

    def keep_part(l, j, h):
        @pl.loop(0, RP // TILE)
        def _(r):
            rows = pl.ds(pl.multiple_of(r * TILE, TILE), TILE)
            for t in range(tiles_across):
                put(r, l, j, h, t, part[rows, pl.ds(t * LANES, LANES)])

    def add_squares():
        def square(r, sums):
            rows = pl.ds(pl.multiple_of(r * TILE, TILE), TILE)
            for t in range(tiles_across):
                x = part[rows, pl.ds(t * LANES, LANES)]
                sums = sums + x * x
            return sums

        squares[...] = lax.fori_loop(0, RP // TILE, square, squares[...])

    def owner_of(way, s):
        return half + s if way == 0 else half - 1 - s

    def tot_copy(way, s, p):
        return pltpu.make_async_remote_copy(
            rx.at[way, s, p], tot.at[p], tot_send.at[s, p], tot_recv.at[p],
            device_id={"dp": owner_of(way, s) * CORES + core}, device_id_type=MESH,
        )

    steps = half * pieces
    squares[...] = jnp.zeros_like(squares)

    def stream(way, t):
        hops = chip if way == 0 else C - 1 - chip
        n = t - LAG * hops
        s, p = n // pieces, lax.rem(n, pieces)
        l, j, h = parts_of(p)

        @pl.when((n >= 0) & (n < steps))
        def _():
            product(owner_of(way, s), l, j, h)

            @pl.when(hops > 0)
            def _():
                add_received(way, s, p)

            @pl.when(hops == C - 1)
            def _():
                add_squares()

            last = (hops == C - 1) & (s == half - 1)

            @pl.when(last)
            def _():
                keep_part(l, j, h)

            @pl.when(jnp.logical_not(last))
            def _():
                pack(way, s, p)

            @pl.when((hops < C - 1) & (n >= FLIGHT))
            def _():
                before = n - FLIGHT
                rs_copy(way, before // pieces, lax.rem(before, pieces)).wait_send()

            @pl.when(hops < C - 1)
            def _():
                rs_copy(way, s, p).start()

    totals = (half - 1) * pieces
    leave = max(steps, totals + LAG * (C - 1))
    early, middle = min(EARLY, totals), min(EARLY + MIDDLE, totals)

    def at_sink(way):
        return chip == (C - 1 if way == 0 else 0)

    def wait_total(n):
        for way in range(2):
            @pl.when(at_sink(way))
            def _():
                tot_copy(way, n // pieces, lax.rem(n, pieces)).wait_send()

    def send_totals(first_one, stop, gated):
        @pl.loop(first_one, stop)
        def _(n):
            if gated:
                wait_total(n - FLIGHT)
            for way in range(2):
                @pl.when(at_sink(way))
                def _():
                    tot_copy(way, n // pieces, lax.rem(n, pieces)).start()

    @pl.loop(0, steps + LAG * (C - 1))
    def _(t):
        l, j, h = parts_of(t)

        @pl.when((t < pieces) & (h == 0))
        def _():
            @pl.when(j == 0)
            def _():
                for c in sorted({half - 1, half}):
                    a_local(l, c).wait()
                    a_remote(l, c).wait_recv()

            b_local(l, j).wait()
            b_remote(l, j).wait_recv()

        @pl.when((t >= pieces) & (t < pieces + L))
        def _():
            for c in range(C):
                if c not in (half - 1, half):
                    a_local(t - pieces, c).wait()
                    a_remote(t - pieces, c).wait_recv()

        stream(0, t)
        stream(1, t)

        @pl.when(t == leave)
        def _():
            send_totals(0, early, False)

    norm[me] = jnp.sum(squares[...], axis=0, keepdims=True)

    def norm_copy(k, slot):
        return pltpu.make_async_remote_copy(
            norm.at[slot], norm.at[slot], norm_send.at[k], norm_recv.at[k],
            device_id=device(k), device_id_type=MESH,
        )

    at_end = (chip == 0) | (chip == C - 1)

    def from_end(k):
        other = lax.rem(lax.rem(me - k + count, count), n_dp) // CORES
        return (other == 0) | (other == C - 1)

    @pl.when(at_end)
    def _():
        @pl.loop(1, count)
        def _(k):
            norm_copy(k, me).start()

    send_totals(early, middle, False)

    @pl.loop(1, count)
    def _(k):
        @pl.when(from_end(k))
        def _():
            norm_copy(k, lax.rem(me - k + count, count)).wait_recv()

    send_totals(middle, totals, True)

    total = None
    for a in range(n_tp):
        for c in sorted({0, C - 1}):
            for k in range(CORES):
                row = norm[a * n_dp + c * CORES + k]
                total = row if total is None else total + row
    total = jnp.sum(total, axis=1, keepdims=True)
    limit = limit_scale * math.sqrt(R * L * N * count)
    clip = limit / jnp.maximum(jnp.sqrt(total), limit)
    block = 8
    clip = jnp.broadcast_to(clip, (block * group, LANES))

    def place(c, q):
        return unit((c * CORES + core) * R, q)

    def ag_copy(way, c, q):
        to = chip + 1 if way == 0 else chip - 1
        return pltpu.make_async_remote_copy(
            wide.at[c, q], wide.at[c, q], ag_send.at[way, c, q], ag_recv.at[c, q],
            device_id={"dp": to * CORES + core}, device_id_type=MESH,
        )

    def local_copy(c, q):
        return pltpu.make_async_copy(wide.at[c, q], weights.at[place(c, q)], out_local.at[c, q])

    def partner_copy(c, q):
        return pltpu.make_async_remote_copy(
            wide.at[c, q], weights.at[place(c, q)], out_send.at[c, q], out_recv.at[c, q],
            device_id=partner, device_id_type=MESH,
        )

    def partner_place(c, q):
        return unit((c * CORES + 1 - core) * R, q)

    def partner_arrival(c, q):
        return pltpu.make_async_remote_copy(
            wide.at[c, q], weights.at[partner_place(c, q)], out_send.at[c, q], out_recv.at[c, q],
            device_id=partner, device_id_type=MESH,
        )

    def update(q):
        slot, j = lax.rem(q, STATE_SLOTS), q // SPLIT

        @pl.when(jnp.logical_not(at_end) & (lax.rem(q, SPLIT // SP) == 0))
        def _():
            for l in range(L):
                p = q // (SPLIT // SP) * L + l
                h = lax.rem(q, SP)
                tot_copy(0, 0, p).wait_recv()
                scale = tot[p, tiles].astype(jnp.float32) * (1.0 / TOP)

                @pl.loop(0, RP // TILE)
                def _(r):
                    for t in range(tiles_across):
                        put(r, l, j, h, t, decode(tot[p, r * tiles_across + t], scale))

        for i in range(3):
            state_load(i, q).wait()

        @pl.loop(0, rows_u // block)
        def _(b):
            here = pl.ds(pl.multiple_of(b * block, block), block)
            start = (j * R + lax.rem(q, SPLIT) * rows_u + b * block) * group
            there = pl.ds(pl.multiple_of(start, block * group), block * group)

            def read(i):
                return state[i, slot, here].reshape(block * group, LANES)

            def write(i, value):
                state[i, slot, here] = value.reshape(block, group, LANES)

            clipped = clip * grad[there, :]
            moment = beta_first * read(1) + (1.0 - beta_first) * clipped
            spread = beta_second * read(2) + (1.0 - beta_second) * clipped * clipped
            old = read(0)
            direction = moment / first_fix / (jnp.sqrt(spread / second_fix) + epsilon)
            new = old - learn_rate * (direction + decay_rate * old)
            write(0, new)
            write(1, moment)
            write(2, spread)
            wide[chip, q, here] = new.astype(jnp.bfloat16).reshape(block, group, LANES)

        @pl.when(chip > 0)
        def _():
            ag_copy(1, chip, q).start()

        @pl.when(chip < C - 1)
        def _():
            ag_copy(0, chip, q).start()

        for i in range(3):
            state_store(i, q).start()
        local_copy(chip, q).start()
        partner_copy(chip, q).start()

        @pl.when((q > 0) & (q - 1 + STATE_SLOTS < d.PQ))
        def _():
            for i in range(3):
                state_store(i, q - 1).wait()
                state_load(i, q - 1 + STATE_SLOTS).start()

    def pass_on(way, c, q):
        ag_copy(way, c, q).wait_recv()

        @pl.when(chip < C - 1 if way == 0 else chip > 0)
        def _():
            ag_copy(way, c, q).start()

        local_copy(c, q).start()
        partner_copy(c, q).start()

    def relay(way, t):
        room = chip if way == 0 else C - 1 - chip
        chunk, q = (t - BEHIND) // (d.PQ + BEHIND), lax.rem(t - BEHIND, d.PQ + BEHIND)
        near = chip - 1 - chunk if way == 0 else chip + 1 + chunk

        @pl.when((t >= BEHIND) & (chunk < room - 1) & (q < d.PQ))
        def _():
            pass_on(way, near, q)

        late = t - jnp.maximum(room - 1, half - 1) * d.PQ - BEHIND * room

        @pl.when((room > 0) & (late >= 0) & (late < d.PQ))
        def _():
            pass_on(way, 0 if way == 0 else C - 1, late)

    @pl.loop(0, (C - 1) * (d.PQ + BEHIND))
    def _(u):
        @pl.when(u < d.PQ)
        def _():
            update(u)

        relay(0, u)
        relay(1, u)

    for q in range(max(0, d.PQ - STATE_SLOTS), d.PQ):
        for i in range(3):
            state_store(i, jnp.int32(q)).wait()

    for l in range(L):
        for c in range(C):
            a_remote(l, c).wait_send()
        for j in range(NB):
            b_remote(l, j).wait_send()

    @pl.when(at_end)
    def _():
        @pl.loop(1, count)
        def _(k):
            norm_copy(k, me).wait_send()

    @pl.loop(steps - min(FLIGHT, steps), steps)
    def _(n):
        @pl.when(chip < C - 1)
        def _():
            rs_copy(0, n // pieces, lax.rem(n, pieces)).wait_send()

        @pl.when(chip > 0)
        def _():
            rs_copy(1, n // pieces, lax.rem(n, pieces)).wait_send()

    @pl.loop(0, totals)
    def _(n):
        @pl.when((n < middle - FLIGHT) | (n >= totals - FLIGHT))
        def _():
            wait_total(n)

    @pl.loop(0, C)
    def _(c):
        @pl.loop(0, d.PQ)
        def _(q):
            @pl.when((c <= chip) & (chip < C - 1))
            def _():
                ag_copy(0, c, q).wait_send()

            @pl.when((c >= chip) & (chip > 0))
            def _():
                ag_copy(1, c, q).wait_send()

            local_copy(c, q).wait()
            partner_copy(c, q).wait_send()
            partner_arrival(c, q).wait_recv()


class Sizes:
    pass


def whole_step(acts, grads, master, first, second):
    d = Sizes()
    d.L, d.T, width = acts.shape
    d.N = grads.shape[2]
    d.n_tp, d.n_dp = lax.axis_size("tp"), lax.axis_size("dp")
    d.C = d.n_dp // CORES
    d.R = width // d.n_dp
    d.AW = d.R if d.R % LANES == 0 else CORES * d.R
    d.WC = math.gcd(512, d.N)
    d.NB = d.N // d.WC
    d.PQ = d.NB * SPLIT
    d.SP = SPLIT if d.R % (SPLIT * LANES) == 0 else 1
    d.RP = d.R // d.SP
    pieces = d.L * d.NB * d.SP
    tiles = d.RP // TILE * (d.WC // LANES)
    across = d.L * d.N // LANES
    group = d.L * d.WC // LANES
    count = d.n_tp * d.n_dp
    half = d.C // 2
    packed = (tiles + 1, TILE, LANES)
    hbm = pl.BlockSpec(memory_space=pl.ANY)
    dma = pltpu.SemaphoreType.DMA
    flat = jax.ShapeDtypeStruct((d.R, across, LANES), jnp.float32)
    return pl.pallas_call(
        functools.partial(step_kernel, d),
        out_shape=(flat, flat, flat, jax.ShapeDtypeStruct((d.n_dp * d.R, across, LANES), jnp.bfloat16)),
        in_specs=[hbm] * 5,
        out_specs=[hbm] * 4,
        scratch_shapes=[
            pltpu.VMEM((CORES, d.L, d.C, d.T, d.AW), jnp.bfloat16),
            pltpu.VMEM((CORES, d.L, d.NB, d.T, d.WC), jnp.bfloat16),
            pltpu.VMEM((d.RP, d.WC), jnp.float32),
            pltpu.VMEM((2, half, pieces) + packed, jnp.bfloat16),
            pltpu.VMEM((pieces,) + packed, jnp.bfloat16),
            pltpu.VMEM((d.NB * d.R * group, LANES), jnp.float32),
            pltpu.VMEM((d.C, d.PQ, d.R // SPLIT, group, LANES), jnp.bfloat16),
            pltpu.VMEM((3, STATE_SLOTS, d.R // SPLIT, group, LANES), jnp.float32),
            pltpu.VMEM((TILE, LANES), jnp.float32),
            pltpu.VMEM((count, 1, LANES), jnp.float32),
            dma((d.L, d.C)), dma((d.L, d.C)), dma((d.L, d.C)),
            dma((d.L, d.NB)), dma((d.L, d.NB)), dma((d.L, d.NB)),
            dma((2, half, pieces)), dma((2, half, pieces)),
            dma((half, pieces)), dma((pieces,)),
            dma((count,)), dma((count,)),
            dma((3, STATE_SLOTS)), dma((3, STATE_SLOTS)),
            dma((2, d.C, d.PQ)), dma((d.C, d.PQ)),
            dma((d.C, d.PQ)), dma((d.C, d.PQ)), dma((d.C, d.PQ)),
        ],
        compiler_params=pltpu.CompilerParams(
            collective_id=0, has_side_effects=True, vmem_limit_bytes=67043328
        ),
        name="whole_step",
    )(acts, grads, master, first, second)


def to_rows(x):
    r, l, n = x.shape
    return x.reshape(r, l, n // LANES, LANES).transpose(0, 2, 1, 3).reshape(r, -1, LANES)


def from_rows(y, l, n):
    return y.reshape(-1, n // LANES, l, LANES).transpose(0, 2, 1, 3).reshape(-1, l, n)


def on_device(activations, out_grads, master, first_moment, second_moment):
    states = [to_rows(x) for x in (master, first_moment, second_moment)]
    outs = whole_step(activations, out_grads, *states)
    return tuple(from_rows(y, *master.shape[1:]) for y in outs)


def solution(mesh):
    return jax.shard_map(
        on_device,
        mesh=mesh,
        in_specs=(
            P(None, "dp", "tp"),
            P(None, "dp", None),
            P(("tp", "dp"), None, None),
            P(("tp", "dp"), None, None),
            P(("tp", "dp"), None, None),
        ),
        out_specs=(
            P(("tp", "dp"), None, None),
            P(("tp", "dp"), None, None),
            P(("tp", "dp"), None, None),
            P("tp", None, None),
        ),
        check_vma=False,
    )
```

```python
import functools
import math

import jax
import jax.numpy as jnp
from jax import lax
from jax.experimental import pallas as pl
from jax.experimental.pallas import tpu as pltpu
from jax.sharding import PartitionSpec as P

beta_first = 0.9
beta_second = 0.95
first_fix = 1.0 - 0.9**10
second_fix = 1.0 - 0.95**10
learn_rate = 0.01
decay_rate = 0.1
epsilon = 1e-08
limit_scale = 2.0
MESH = pl.DeviceIdType.MESH
CORES = 2
LANES = 128
TILE = 16
TOP = 224.0
STATE_SLOTS = 4
LAG = 2
SPLIT = 2
BEHIND = 3
EARLY, MIDDLE = 3, 3
TAIL = 3
FLIGHT = 2


def decode(code, scale):
    code = code.astype(jnp.float32)
    size = jnp.abs(code)
    root = jnp.exp(jnp.log(jnp.maximum(size, 1e-37)) * (1.0 / 16.0))
    root = jnp.where(size > 0.0, root, 0.0)
    return jnp.where(code < 0.0, -root, root) * scale


def encode(value, shrink):
    x = value * shrink
    power = x * x
    power = power * power
    power = power * power
    power = power * power
    return jnp.where(x < 0.0, -power, power).astype(jnp.bfloat16)


def step_kernel(
    d,
    acts, grads, master, first, second,
    new_master, new_first, new_second, weights, tail,
    a_buf, b_buf, part, rx, tot, grad, wide, state, squares, norm,
    a_own, a_send, a_recv, b_own, b_send, b_recv,
    rs_send, rs_recv, tot_send, tot_recv, norm_send, norm_recv, state_in, state_out,
    ag_send, ag_recv, out_local, out_send, out_recv, tail_sem,
):
    L, T, R, N, C, AW, WC, NB = d.L, d.T, d.R, d.N, d.C, d.AW, d.WC, d.NB
    n_tp, n_dp = d.n_tp, d.n_dp
    SP, RP = d.SP, d.RP
    pieces, tiles_across, lane_tiles = L * NB * SP, WC // LANES, N // LANES
    tiles = RP // TILE * tiles_across
    group = tiles_across * L
    half, rows_u = C // 2, R // SPLIT
    index = lax.axis_index("dp")
    chip, core = index // CORES, lax.rem(index, CORES)
    partner = {"dp": chip * CORES + 1 - core}
    me = lax.axis_index("tp") * n_dp + index
    count = n_tp * n_dp

    def column(c, k):
        start = c * CORES * R + (k * R if AW == R else 0)
        return pl.ds(pl.multiple_of(start, LANES), AW)

    def a_local(l, c):
        return pltpu.make_async_copy(
            acts.at[l, :, column(c, core)], a_buf.at[0, l, c], a_own.at[l, c]
        )

    def a_remote(l, c):
        return pltpu.make_async_remote_copy(
            acts.at[l, :, column(c, 1 - core)], a_buf.at[1, l, c],
            a_send.at[l, c], a_recv.at[l, c],
            device_id=partner, device_id_type=MESH,
        )

    def b_columns(j):
        return pl.ds(pl.multiple_of(j * WC, LANES), WC)

    def b_local(l, j):
        return pltpu.make_async_copy(
            grads.at[l, :, b_columns(j)], b_buf.at[0, l, j], b_own.at[l, j]
        )

    def b_remote(l, j):
        return pltpu.make_async_remote_copy(
            grads.at[l, :, b_columns(j)], b_buf.at[1, l, j],
            b_send.at[l, j], b_recv.at[l, j],
            device_id=partner, device_id_type=MESH,
        )

    def in_order(a_copy, b_copy):
        for l in range(L):
            for c in sorted({half - 1, half}):
                a_copy(l, c).start()
        for j in range(NB):
            for l in range(L):
                b_copy(l, j).start()
        for c in range(C):
            if c not in (half - 1, half):
                for l in range(L):
                    a_copy(l, c).start()

    in_order(a_local, b_local)

    sources = (master, first, second)
    targets = (new_master, new_first, new_second)

    def unit(start, q):
        rows = start + lax.rem(q, SPLIT) * rows_u
        return (
            pl.ds(pl.multiple_of(rows, TILE), rows_u),
            pl.ds(pl.multiple_of(q // SPLIT * group, group), group),
        )

    def state_load(i, q):
        slot = lax.rem(q, STATE_SLOTS)
        return pltpu.make_async_copy(
            sources[i].at[unit(0, q)], state.at[i, slot], state_in.at[i, slot]
        )

    def state_store(i, q):
        slot = lax.rem(q, STATE_SLOTS)
        return pltpu.make_async_copy(
            state.at[i, slot], targets[i].at[unit(0, q)], state_out.at[i, slot]
        )

    barrier = pltpu.get_barrier_semaphore()

    def device(k):
        other = lax.rem(me + k, count)
        return {"tp": other // n_dp, "dp": lax.rem(other, n_dp)}

    @pl.loop(1, count)
    def _(k):
        pl.semaphore_signal(barrier, inc=1, device_id=device(k), device_id_type=MESH)

    pl.semaphore_wait(barrier, count - 1)

    in_order(a_remote, b_remote)

    for q in range(min(STATE_SLOTS, d.PQ)):
        for i in range(3):
            state_load(i, jnp.int32(q)).start()

    def parts_of(p):
        return lax.rem(p, L), p // (L * SP), lax.rem(p // L, SP)

    def product(c, l, j, h):
        total = None
        for w in range(CORES):
            if SP == 1:
                lhs = a_buf[w, l, c]
            else:
                lhs = a_buf[w, l, c, :, pl.ds(pl.multiple_of(h * RP, LANES), RP)]
            if AW != R:
                lhs = jnp.where(core == 0, lhs[:, :R], lhs[:, R:])
            term = lax.dot_general(
                lhs, b_buf[w, l, j], (((0,), (0,)), ((), ())),
                preferred_element_type=jnp.float32,
            )
            total = term if total is None else total + term
        part[...] = total

    def rs_copy(way, s, p):
        to = chip + 1 if way == 0 else chip - 1
        return pltpu.make_async_remote_copy(
            rx.at[way, s, p], rx.at[way, s, p],
            rs_send.at[way, s, p], rs_recv.at[way, s, p],
            device_id={"dp": to * CORES + core}, device_id_type=MESH,
        )

    def add_received(way, s, p):
        rs_copy(way, s, p).wait_recv()
        scale = rx[way, s, p, tiles].astype(jnp.float32) * (1.0 / TOP)

        @pl.loop(0, RP // TILE)
        def _(r):
            rows = pl.ds(pl.multiple_of(r * TILE, TILE), TILE)
            for t in range(tiles_across):
                lanes = pl.ds(t * LANES, LANES)
                code = rx[way, s, p, r * tiles_across + t]
                part[rows, lanes] += decode(code, scale)

    def pack(way, s, p):
        def widest(r, top):
            rows = pl.ds(pl.multiple_of(r * TILE, TILE), TILE)
            for t in range(tiles_across):
                top = jnp.maximum(top, jnp.abs(part[rows, pl.ds(t * LANES, LANES)]))
            return top

        top = lax.fori_loop(0, RP // TILE, widest, jnp.zeros((TILE, LANES), jnp.float32))
        top = jnp.maximum(top, 1e-25).astype(jnp.bfloat16)
        rx[way, s, p, tiles] = top
        shrink = TOP / top.astype(jnp.float32)

        @pl.loop(0, RP // TILE)
        def _(r):
            rows = pl.ds(pl.multiple_of(r * TILE, TILE), TILE)
            for t in range(tiles_across):
                value = part[rows, pl.ds(t * LANES, LANES)]
                rx[way, s, p, r * tiles_across + t] = encode(value, shrink)

    def put(r, l, j, h, t, value):
        for k in range(TILE // 8):
            start = (j * R + h * RP + r * TILE + k * 8) * group + t * L + l
            grad[pl.ds(start, 8, stride=group), :] = value[k * 8 : k * 8 + 8]

    def keep_part(l, j, h):
        @pl.loop(0, RP // TILE)
        def _(r):
            rows = pl.ds(pl.multiple_of(r * TILE, TILE), TILE)
            for t in range(tiles_across):
                put(r, l, j, h, t, part[rows, pl.ds(t * LANES, LANES)])

    def add_squares():
        def square(r, sums):
            rows = pl.ds(pl.multiple_of(r * TILE, TILE), TILE)
            for t in range(tiles_across):
                x = part[rows, pl.ds(t * LANES, LANES)]
                sums = sums + x * x
            return sums

        squares[...] = lax.fori_loop(0, RP // TILE, square, squares[...])

    def owner_of(way, s):
        return half + s if way == 0 else half - 1 - s

    def tot_copy(way, s, p):
        return pltpu.make_async_remote_copy(
            rx.at[way, s, p], tot.at[p], tot_send.at[s, p], tot_recv.at[p],
            device_id={"dp": owner_of(way, s) * CORES + core}, device_id_type=MESH,
        )

    steps = half * pieces
    squares[...] = jnp.zeros_like(squares)

    def stream(way, t):
        hops = chip if way == 0 else C - 1 - chip
        n = t - LAG * hops
        s, p = n // pieces, lax.rem(n, pieces)
        l, j, h = parts_of(p)

        @pl.when((n >= 0) & (n < steps))
        def _():
            product(owner_of(way, s), l, j, h)

            @pl.when(hops > 0)
            def _():
                add_received(way, s, p)

            @pl.when(hops == C - 1)
            def _():
                add_squares()

            last = (hops == C - 1) & (s == half - 1)

            @pl.when(last)
            def _():
                keep_part(l, j, h)

            @pl.when(jnp.logical_not(last))
            def _():
                pack(way, s, p)

            @pl.when((hops < C - 1) & (n >= FLIGHT))
            def _():
                before = n - FLIGHT
                rs_copy(way, before // pieces, lax.rem(before, pieces)).wait_send()

            @pl.when(hops < C - 1)
            def _():
                rs_copy(way, s, p).start()

    totals = (half - 1) * pieces
    leave = max(steps, totals + LAG * (C - 1))
    early, middle = min(EARLY, totals), min(EARLY + MIDDLE, totals)

    def at_sink(way):
        return chip == (C - 1 if way == 0 else 0)

    def wait_total(n):
        for way in range(2):
            @pl.when(at_sink(way))
            def _():
                tot_copy(way, n // pieces, lax.rem(n, pieces)).wait_send()

    def send_totals(first_one, stop, gated):
        @pl.loop(first_one, stop)
        def _(n):
            if gated:
                wait_total(n - FLIGHT)
            for way in range(2):
                @pl.when(at_sink(way))
                def _():
                    tot_copy(way, n // pieces, lax.rem(n, pieces)).start()

    @pl.loop(0, steps + LAG * (C - 1))
    def _(t):
        l, j, h = parts_of(t)

        @pl.when((t < pieces) & (h == 0))
        def _():
            @pl.when(j == 0)
            def _():
                for c in sorted({half - 1, half}):
                    a_local(l, c).wait()
                    a_remote(l, c).wait_recv()

            b_local(l, j).wait()
            b_remote(l, j).wait_recv()

        @pl.when((t >= pieces) & (t < pieces + L))
        def _():
            for c in range(C):
                if c not in (half - 1, half):
                    a_local(t - pieces, c).wait()
                    a_remote(t - pieces, c).wait_recv()

        stream(0, t)
        stream(1, t)

        @pl.when(t == leave)
        def _():
            send_totals(0, early, False)

    norm[me] = jnp.sum(squares[...], axis=0, keepdims=True)

    def norm_copy(k, slot):
        return pltpu.make_async_remote_copy(
            norm.at[slot], norm.at[slot], norm_send.at[k], norm_recv.at[k],
            device_id=device(k), device_id_type=MESH,
        )

    at_end = (chip == 0) | (chip == C - 1)

    def from_end(k):
        other = lax.rem(lax.rem(me - k + count, count), n_dp) // CORES
        return (other == 0) | (other == C - 1)

    @pl.when(at_end)
    def _():
        @pl.loop(1, count)
        def _(k):
            norm_copy(k, me).start()

    send_totals(early, middle, False)

    @pl.loop(1, count)
    def _(k):
        @pl.when(from_end(k))
        def _():
            norm_copy(k, lax.rem(me - k + count, count)).wait_recv()

    send_totals(middle, totals, True)

    total = None
    for a in range(n_tp):
        for c in sorted({0, C - 1}):
            for k in range(CORES):
                row = norm[a * n_dp + c * CORES + k]
                total = row if total is None else total + row
    total = jnp.sum(total, axis=1, keepdims=True)
    limit = limit_scale * math.sqrt(R * L * N * count)
    clip = limit / jnp.maximum(jnp.sqrt(total), limit)
    block = 8
    clip = jnp.broadcast_to(clip, (block * group, LANES))

    def place(c, q):
        return unit((c * CORES + core) * R, q)

    def ag_copy(way, c, q):
        to = chip + 1 if way == 0 else chip - 1
        return pltpu.make_async_remote_copy(
            wide.at[c, q], wide.at[c, q], ag_send.at[way, c, q], ag_recv.at[c, q],
            device_id={"dp": to * CORES + core}, device_id_type=MESH,
        )

    def local_copy(c, q):
        return pltpu.make_async_copy(wide.at[c, q], weights.at[place(c, q)], out_local.at[c, q])

    def partner_copy(c, q):
        return pltpu.make_async_remote_copy(
            wide.at[c, q], weights.at[place(c, q)], out_send.at[c, q], out_recv.at[c, q],
            device_id=partner, device_id_type=MESH,
        )

    def partner_place(c, q):
        return unit((c * CORES + 1 - core) * R, q)

    def partner_arrival(c, q):
        return pltpu.make_async_remote_copy(
            wide.at[c, q], weights.at[partner_place(c, q)], out_send.at[c, q], out_recv.at[c, q],
            device_id=partner, device_id_type=MESH,
        )

    first_tail = d.PQ - d.TAIL

    def is_tail(way, c, q, at):
        if way == 0:
            return (q >= first_tail) & (c == 0) & (at == C - 2)
        return (q >= first_tail) & (c == C - 1) & (at == 1)

    def tail_copy(c, q):
        return pltpu.make_async_copy(
            wide.at[c, q], tail.at[q - first_tail], tail_sem.at[q - first_tail]
        )

    def hand_on(way, c, q):
        left = is_tail(way, c, q, chip)

        @pl.when((chip < C - 1 if way == 0 else chip > 0) & jnp.logical_not(left))
        def _():
            ag_copy(way, c, q).start()

        @pl.when(left)
        def _():
            tail_copy(c, q).start()

    def update(q):
        slot, j = lax.rem(q, STATE_SLOTS), q // SPLIT

        @pl.when(jnp.logical_not(at_end) & (lax.rem(q, SPLIT // SP) == 0))
        def _():
            for l in range(L):
                p = q // (SPLIT // SP) * L + l
                h = lax.rem(q, SP)
                tot_copy(0, 0, p).wait_recv()
                scale = tot[p, tiles].astype(jnp.float32) * (1.0 / TOP)

                @pl.loop(0, RP // TILE)
                def _(r):
                    for t in range(tiles_across):
                        put(r, l, j, h, t, decode(tot[p, r * tiles_across + t], scale))

        for i in range(3):
            state_load(i, q).wait()

        @pl.loop(0, rows_u // block)
        def _(b):
            here = pl.ds(pl.multiple_of(b * block, block), block)
            start = (j * R + lax.rem(q, SPLIT) * rows_u + b * block) * group
            there = pl.ds(pl.multiple_of(start, block * group), block * group)

            def read(i):
                return state[i, slot, here].reshape(block * group, LANES)

            def write(i, value):
                state[i, slot, here] = value.reshape(block, group, LANES)

            clipped = clip * grad[there, :]
            moment = beta_first * read(1) + (1.0 - beta_first) * clipped
            spread = beta_second * read(2) + (1.0 - beta_second) * clipped * clipped
            old = read(0)
            direction = moment / first_fix / (jnp.sqrt(spread / second_fix) + epsilon)
            new = old - learn_rate * (direction + decay_rate * old)
            write(0, new)
            write(1, moment)
            write(2, spread)
            wide[chip, q, here] = new.astype(jnp.bfloat16).reshape(block, group, LANES)

        hand_on(1, chip, q)
        hand_on(0, chip, q)
        for i in range(3):
            state_store(i, q).start()
        local_copy(chip, q).start()
        partner_copy(chip, q).start()

        @pl.when((q > 0) & (q - 1 + STATE_SLOTS < d.PQ))
        def _():
            for i in range(3):
                state_store(i, q - 1).wait()
                state_load(i, q - 1 + STATE_SLOTS).start()

    def pass_on(way, c, q):
        @pl.when(jnp.logical_not(is_tail(way, c, q, chip - 1 if way == 0 else chip + 1)))
        def _():
            ag_copy(way, c, q).wait_recv()
            hand_on(way, c, q)
            local_copy(c, q).start()
            partner_copy(c, q).start()

    def relay(way, t):
        room = chip if way == 0 else C - 1 - chip
        chunk, q = (t - BEHIND) // (d.PQ + BEHIND), lax.rem(t - BEHIND, d.PQ + BEHIND)
        near = chip - 1 - chunk if way == 0 else chip + 1 + chunk

        @pl.when((t >= BEHIND) & (chunk < room - 1) & (q < d.PQ))
        def _():
            pass_on(way, near, q)

        late = t - jnp.maximum(room - 1, half - 1) * d.PQ - BEHIND * room

        @pl.when((room > 0) & (late >= 0) & (late < d.PQ))
        def _():
            pass_on(way, 0 if way == 0 else C - 1, late)

    @pl.loop(0, (C - 1) * (d.PQ + BEHIND))
    def _(u):
        @pl.when(u < d.PQ)
        def _():
            update(u)

        relay(0, u)
        relay(1, u)

    for q in range(max(0, d.PQ - STATE_SLOTS), d.PQ):
        for i in range(3):
            state_store(i, jnp.int32(q)).wait()

    for l in range(L):
        for c in range(C):
            a_remote(l, c).wait_send()
        for j in range(NB):
            b_remote(l, j).wait_send()

    @pl.when(at_end)
    def _():
        @pl.loop(1, count)
        def _(k):
            norm_copy(k, me).wait_send()

    @pl.loop(steps - min(FLIGHT, steps), steps)
    def _(n):
        @pl.when(chip < C - 1)
        def _():
            rs_copy(0, n // pieces, lax.rem(n, pieces)).wait_send()

        @pl.when(chip > 0)
        def _():
            rs_copy(1, n // pieces, lax.rem(n, pieces)).wait_send()

    @pl.loop(0, totals)
    def _(n):
        @pl.when((n < middle - FLIGHT) | (n >= totals - FLIGHT))
        def _():
            wait_total(n)

    @pl.loop(0, C)
    def _(c):
        @pl.loop(0, d.PQ)
        def _(q):
            for way in range(2):
                left = is_tail(way, c, q, chip)
                sent = (c <= chip) & (chip < C - 1) if way == 0 else (c >= chip) & (chip > 0)

                @pl.when(sent & jnp.logical_not(left))
                def _():
                    ag_copy(way, c, q).wait_send()

                @pl.when(left)
                def _():
                    tail_copy(c, q).wait()

            missing = is_tail(0, c, q, chip - 1) | is_tail(1, c, q, chip + 1)

            @pl.when(jnp.logical_not(missing))
            def _():
                local_copy(c, q).wait()
                partner_copy(c, q).wait_send()
                partner_arrival(c, q).wait_recv()


class Sizes:
    pass


def whole_step(acts, grads, master, first, second):
    d = Sizes()
    d.L, d.T, width = acts.shape
    d.N = grads.shape[2]
    d.n_tp, d.n_dp = lax.axis_size("tp"), lax.axis_size("dp")
    d.C = d.n_dp // CORES
    d.R = width // d.n_dp
    d.AW = d.R if d.R % LANES == 0 else CORES * d.R
    d.WC = math.gcd(512, d.N)
    d.NB = d.N // d.WC
    d.PQ = d.NB * SPLIT
    d.TAIL = min(TAIL, d.PQ)
    d.SP = SPLIT if d.R % (SPLIT * LANES) == 0 else 1
    d.RP = d.R // d.SP
    pieces = d.L * d.NB * d.SP
    tiles = d.RP // TILE * (d.WC // LANES)
    across = d.L * d.N // LANES
    group = d.L * d.WC // LANES
    count = d.n_tp * d.n_dp
    half = d.C // 2
    packed = (tiles + 1, TILE, LANES)
    hbm = pl.BlockSpec(memory_space=pl.ANY)
    dma = pltpu.SemaphoreType.DMA
    flat = jax.ShapeDtypeStruct((d.R, across, LANES), jnp.float32)
    outs = pl.pallas_call(
        functools.partial(step_kernel, d),
        out_shape=(
            flat, flat, flat,
            jax.ShapeDtypeStruct((d.n_dp * d.R, across, LANES), jnp.bfloat16),
            jax.ShapeDtypeStruct((d.TAIL, d.R // SPLIT, group, LANES), jnp.bfloat16),
        ),
        in_specs=[hbm] * 5,
        out_specs=[hbm] * 5,
        scratch_shapes=[
            pltpu.VMEM((CORES, d.L, d.C, d.T, d.AW), jnp.bfloat16),
            pltpu.VMEM((CORES, d.L, d.NB, d.T, d.WC), jnp.bfloat16),
            pltpu.VMEM((d.RP, d.WC), jnp.float32),
            pltpu.VMEM((2, half, pieces) + packed, jnp.bfloat16),
            pltpu.VMEM((pieces,) + packed, jnp.bfloat16),
            pltpu.VMEM((d.NB * d.R * group, LANES), jnp.float32),
            pltpu.VMEM((d.C, d.PQ, d.R // SPLIT, group, LANES), jnp.bfloat16),
            pltpu.VMEM((3, STATE_SLOTS, d.R // SPLIT, group, LANES), jnp.float32),
            pltpu.VMEM((TILE, LANES), jnp.float32),
            pltpu.VMEM((count, 1, LANES), jnp.float32),
            dma((d.L, d.C)), dma((d.L, d.C)), dma((d.L, d.C)),
            dma((d.L, d.NB)), dma((d.L, d.NB)), dma((d.L, d.NB)),
            dma((2, half, pieces)), dma((2, half, pieces)),
            dma((half, pieces)), dma((pieces,)),
            dma((count,)), dma((count,)),
            dma((3, STATE_SLOTS)), dma((3, STATE_SLOTS)),
            dma((2, d.C, d.PQ)), dma((d.C, d.PQ)),
            dma((d.C, d.PQ)), dma((d.C, d.PQ)), dma((d.C, d.PQ)),
            dma((d.TAIL,)),
        ],
        compiler_params=pltpu.CompilerParams(
            collective_id=0, has_side_effects=True, vmem_limit_bytes=67043328
        ),
        name="whole_step",
    )(acts, grads, master, first, second)
    return d, outs


def copy_kernel(count, *refs):
    sources, targets = refs[:count], refs[count : 2 * count]
    for source, target in zip(sources, targets):
        target[...] = source[...]


def copy_out(arrays):
    blocks = 8

    def spec(x):
        return pl.BlockSpec((x.shape[0] // blocks,) + x.shape[1:], lambda b: (b, 0, 0))

    moved = 2 * sum(x.size * x.dtype.itemsize for x in arrays)
    return pl.pallas_call(
        functools.partial(copy_kernel, len(arrays)),
        grid=(blocks,),
        out_shape=[jax.ShapeDtypeStruct(x.shape, x.dtype) for x in arrays],
        in_specs=[spec(x) for x in arrays],
        out_specs=[spec(x) for x in arrays],
        cost_estimate=pl.CostEstimate(flops=0, bytes_accessed=moved, transcendentals=0),
        compiler_params=pltpu.CompilerParams(vmem_limit_bytes=56 * 2**20),
        name="copy_out",
    )(*arrays)


def insert_kernel(d, own, other, before, weights, sems):
    index = lax.axis_index("dp")
    chip, core = index // CORES, lax.rem(index, CORES)
    group, rows_u = own.shape[2], own.shape[1]

    def each(act):
        for n, source in enumerate((own, other)):
            for k in range(d.TAIL):
                q = d.PQ - d.TAIL + k
                c = jnp.where(chip == 0, d.C - 1, 0)
                row = (c * CORES + (core if n == 0 else 1 - core)) * d.R + q % SPLIT * rows_u
                copy = pltpu.make_async_copy(
                    source.at[k],
                    weights.at[pl.ds(row, rows_u), pl.ds(q // SPLIT * group, group)],
                    sems.at[n, k],
                )
                copy.start() if act == 0 else copy.wait()

    @pl.when((chip == 0) | (chip == d.C - 1))
    def _():
        each(0)
        each(1)


def insert(d, own, other, weights):
    hbm, vmem = pl.BlockSpec(memory_space=pl.ANY), pl.BlockSpec(memory_space=pltpu.VMEM)
    return pl.pallas_call(
        functools.partial(insert_kernel, d),
        out_shape=jax.ShapeDtypeStruct(weights.shape, weights.dtype),
        in_specs=[vmem, vmem, hbm],
        out_specs=hbm,
        input_output_aliases={2: 0},
        scratch_shapes=[pltpu.SemaphoreType.DMA((2, d.TAIL))],
        name="insert",
    )(own, other, weights)


def finish(d, outs):
    *arrays, tail = outs
    last = d.C - 1
    hops = [(1, 0), (last - 1, last)]
    pairs = [(a * CORES + k, b * CORES + k) for a, b in hops for k in range(CORES)]
    swap = [(b * CORES + k, b * CORES + 1 - k) for _, b in hops for k in range(CORES)]
    own = lax.ppermute(tail, "dp", pairs)
    arrays = copy_out(arrays)
    own, arrays = lax.optimization_barrier((own, arrays))
    other = lax.ppermute(own, "dp", swap)
    return *arrays[:3], insert(d, own, other, arrays[3])


def to_rows(x):
    r, l, n = x.shape
    return x.reshape(r, l, n // LANES, LANES).transpose(0, 2, 1, 3).reshape(r, -1, LANES)


def from_rows(y, l, n):
    return y.reshape(-1, n // LANES, l, LANES).transpose(0, 2, 1, 3).reshape(-1, l, n)


def on_device(activations, out_grads, master, first_moment, second_moment):
    states = [to_rows(x) for x in (master, first_moment, second_moment)]
    outs = finish(*whole_step(activations, out_grads, *states))
    return tuple(from_rows(y, *master.shape[1:]) for y in outs)


def solution(mesh):
    return jax.shard_map(
        on_device,
        mesh=mesh,
        in_specs=(
            P(None, "dp", "tp"),
            P(None, "dp", None),
            P(("tp", "dp"), None, None),
            P(("tp", "dp"), None, None),
            P(("tp", "dp"), None, None),
        ),
        out_specs=(
            P(("tp", "dp"), None, None),
            P(("tp", "dp"), None, None),
            P(("tp", "dp"), None, None),
            P("tp", None, None),
        ),
        check_vma=False,
    )
```
